16 devices in a mesh: dp: 2 (over y, z), tp: 8 (over x, core).
Axes of the slice: x: 4, y: 2, z: 1, core: 2. Of those that a mesh axis runs over, the one named last changes fastest.
The devices are a block of a 4x4x8 slice.
Arguments:
- hidden: bfloat16 [2, 256, 9216], P('dp'), parts along dimension 0
- ln_gain: float32 [9216], replicated
- ln_bias: float32 [9216], replicated
- embedding: bfloat16 [51200, 9216], P('tp')
- targets: int32 [2, 256], P('dp'), parts along dimension 0
- score_mask: int32 [2, 256], P('dp'), parts along dimension 0
Outputs:
- output 1: float32 [2, 256], P('dp'), parts along dimension 0
- output 2: float32 [2, 256], P('dp'), parts along dimension 0
- output 3: float32 [2], P('dp'), parts along dimension 0
- output 4: float32 [2, 256], P('dp'), parts along dimension 0
There are 2 independent parts. The reference program is written for one: setup_inputs(seed, part) draws one part's arguments, and reference() takes and returns one part's arrays. A program takes and returns all parts, laid end to end along the dimension named above; an argument that names none is the same for every part.
All inputs are finite; a program needn't handle non-finite values.
Results may differ from the reference program's by a relative error of at most 0.001.
Values sent between devices are 32-bit elements.
A program may use at most 768 MiB of HBM per device.

```python
import jax
import jax.numpy as jnp
from jax import lax

BATCH = 1
SEQ_LEN = 256
D_MODEL = 9216
VOCAB = 50272
VOCAB_PAD = 51200
LN_EPS = 1e-5
LOGIT_SCALE = 3.0


def setup_inputs(seed: int = 0, part: int = 0) -> dict:
    part_key = jax.random.fold_in(jax.random.key(seed), part)
    shared_key = jax.random.key(seed + 1)
    key_x, key_tgt, key_lo, key_hi = jax.random.split(part_key, 4)
    key_g, key_b, key_e = jax.random.split(shared_key, 3)
    hidden = jax.random.normal(key_x, (BATCH, SEQ_LEN, D_MODEL), jnp.float32).astype(jnp.bfloat16)
    ln_gain = 1.0 + 0.3 * jax.random.normal(key_g, (D_MODEL,), jnp.float32)
    ln_bias = 0.5 * jax.random.normal(key_b, (D_MODEL,), jnp.float32)
    embedding = (jax.random.normal(key_e, (VOCAB_PAD, D_MODEL), jnp.float32) * (LOGIT_SCALE * D_MODEL ** -0.5)).astype(jnp.bfloat16)
    targets = jax.random.randint(key_tgt, (BATCH, SEQ_LEN), 0, VOCAB, jnp.int32)
    targets = targets.at[0, 0].set(0).at[0, SEQ_LEN - 1].set(VOCAB - 1)
    positions = jnp.arange(SEQ_LEN)[None, :]
    run_start = jax.random.randint(key_lo, (BATCH, 1), 0, SEQ_LEN // 2, jnp.int32)
    run_stop = jax.random.randint(key_hi, (BATCH, 1), SEQ_LEN // 2 + 1, SEQ_LEN + 1, jnp.int32)
    score_mask = ((positions >= run_start) & (positions < run_stop)).astype(jnp.int32)
    return {"hidden": hidden, "ln_gain": ln_gain, "ln_bias": ln_bias, "embedding": embedding, "targets": targets, "score_mask": score_mask}


def reference(hidden, ln_gain, ln_bias, embedding, targets, score_mask):
    vocab_ids = jnp.arange(VOCAB_PAD)
    valid_rows = vocab_ids < VOCAB

    def score_row(row):
        hidden_row, target_row, mask_row = row
        hidden_f = hidden_row.astype(jnp.float32)
        row_mean = jnp.mean(hidden_f, axis=-1, keepdims=True)
        centered = hidden_f - row_mean
        row_var = jnp.mean(centered * centered, axis=-1, keepdims=True)
        normed = (centered * lax.rsqrt(row_var + LN_EPS) * ln_gain + ln_bias).astype(jnp.bfloat16)
        logits = jnp.dot(normed, embedding.T, preferred_element_type=jnp.float32)
        logits = jnp.where(valid_rows[None, :], logits, -jnp.inf)
        row_max = jnp.max(logits, axis=-1)
        log_norm = row_max + jnp.log(jnp.sum(jnp.exp(logits - row_max[:, None]), axis=-1))
        target_logit = jnp.sum(jnp.where(vocab_ids[None, :] == target_row[:, None], logits, 0.0), axis=-1)
        token_logp = (target_logit - log_norm) * mask_row.astype(jnp.float32)
        return log_norm, token_logp, jnp.sum(token_logp), row_max - log_norm

    log_norm, token_logp, seq_score, top_logp = lax.map(score_row, (hidden, targets, score_mask))
    return log_norm, token_logp, seq_score, top_logp
```

```python
import functools

import jax
import jax.numpy as jnp
from jax import lax
from jax.experimental import pallas as pl
from jax.experimental.pallas import tpu as pltpu
from jax.sharding import PartitionSpec as P

OPT_VOCAB = 50272
LN_EPS = 1e-5

TILE = 256
BLOCK = 256
PIECE = 64
LANES = 128
RING = 12
PARTS = 3
HID_PARTS = 4
F32 = jnp.float32


def head_kernel(hid_hbm, gain_hbm, bias_hbm, emb_hbm, tgt_hbm, stats_ref,
                h, ring, z, gain, bias, tgt, mean_b, rstd_b, part, m8, s8, t8, small_sem, hid_sem, ring_sem):
    tokens, width = h.shape
    rows = emb_hbm.shape[0]
    n_blocks = rows // BLOCK
    passes = width // (2 * TILE)
    part_width = width // PARTS
    part_passes = passes // PARTS
    hid_rows = tokens // HID_PARTS
    me = lax.axis_index("tp")
    base = me * rows

    def hid_copy(i):
        at = pl.ds(i * hid_rows, hid_rows)
        return pltpu.make_async_copy(hid_hbm.at[0, at], h.at[at], hid_sem.at[i])

    def ring_copy(b, i):
        slot = lax.rem(b, RING)
        cols = pl.ds(i * part_width, part_width)
        return pltpu.make_async_copy(
            emb_hbm.at[pl.ds(b * BLOCK, BLOCK), cols], ring.at[slot, :, cols], ring_sem.at[slot, i])

    small = [pltpu.make_async_copy(src, dst, small_sem.at[i]) for i, (src, dst) in enumerate(
        ((gain_hbm, gain), (bias_hbm, bias), (tgt_hbm, tgt)))]

    for i in range(HID_PARTS):
        hid_copy(i).start()
    for copy in small:
        copy.start()
    for b in range(min(RING, n_blocks)):
        for i in range(PARTS):
            ring_copy(b, i).start()

    def lane_sum(r, n, fn):
        acc = [jnp.zeros((n, LANES), F32) for _ in range(2)]
        for c in range(width // LANES):
            acc[c % 2] += fn(h[pl.ds(r, n), pl.ds(c * LANES, LANES)].astype(F32))
        return acc[0] + acc[1]

    group = 16

    def mean_rows(i):
        for g in range(hid_rows // group):
            r = i * hid_rows + g * group
            part[pl.ds(r, group)] = lane_sum(r, group, lambda x: x)
        at = pl.ds(i * hid_rows, hid_rows)
        mean = jnp.sum(part[at], axis=-1, keepdims=True) * (1.0 / width)
        mean_b[at] = jnp.broadcast_to(mean, (hid_rows, LANES))

    def var_rows(i):
        for g in range(hid_rows // group):
            r = i * hid_rows + g * group
            mean = mean_b[pl.ds(r, group)]
            part[pl.ds(r, group)] = lane_sum(r, group, lambda x: (x - mean) * (x - mean))
        at = pl.ds(i * hid_rows, hid_rows)
        var = jnp.sum(part[at], axis=-1, keepdims=True) * (1.0 / width)
        rstd_b[at] = jnp.broadcast_to(lax.rsqrt(var + LN_EPS), (hid_rows, LANES))

    for i in range(HID_PARTS):
        hid_copy(i).wait()
        mean_rows(i)
        if i:
            var_rows(i - 1)
    var_rows(HID_PARTS - 1)

    for copy in small:
        copy.wait()
    m8[...] = jnp.full_like(m8, jnp.finfo(F32).min)
    s8[...] = jnp.zeros_like(s8)
    t8[...] = jnp.zeros_like(t8)

    def normalize(k):
        for c in range(TILE // LANES):
            cols = pl.ds(k * TILE + c * LANES, LANES)
            x = h[:, cols].astype(F32)
            x = (x - mean_b[...]) * rstd_b[...] * gain[:, cols] + bias[:, cols]
            h[:, cols] = x.astype(h.dtype)

    def matmuls(*accs):
        n_piece = BLOCK // PIECE
        accs = [[list(accs[(w * 2 + q) * n_piece:(w * 2 + q + 1) * n_piece]) for q in range(2)] for w in range(2)]

        for which in accs:
            for q in which:
                for acc in q:
                    z[pl.ds(0, PIECE)] = pltpu.matmul_pop(acc)

        def push(j, q):
            k = 2 * j + q
            pltpu.matmul_push_rhs(h[:, pl.ds(k * TILE, TILE)], staging_register=j % 2, mxu_index=q, transpose=True)

        def accumulate(b, j, q, which):
            slot = lax.rem(b, RING)
            cols = pl.ds((2 * j + q) * TILE, TILE)
            for p in range(n_piece):
                lhs = ring[slot, pl.ds(p * PIECE, PIECE), cols]
                pltpu.matmul_acc_lhs(accs[which][q][p], lhs, load_staged_rhs=j % 2 if p == 0 else None)

        def drain(b, which, first, last):
            offset = base + b * BLOCK
            target = tgt[...] - offset
            limit = OPT_VOCAB - offset
            top, picked = m8[1], t8[...]
            for p in range(first, last):
                logits = pltpu.matmul_pop(accs[which][0][p]) + pltpu.matmul_pop(accs[which][1][p])
                row = lax.broadcasted_iota(jnp.int32, logits.shape, 0) + p * PIECE
                logits = jnp.where(row < limit, logits, -jnp.inf)
                z[pl.ds(p * PIECE, PIECE)] = logits
                top = jnp.maximum(top, jnp.max(logits.reshape(PIECE // 8, 8, tokens), axis=0))
                hit = jnp.where(row == target, logits, 0.0)
                picked = picked + jnp.sum(hit.reshape(PIECE // 8, 8, tokens), axis=0)
            m8[1] = top
            t8[...] = picked

        def exps(first, last):
            top = m8[1]
            total = s8[...]
            if first == 0:
                total = total * jnp.exp(m8[0] - top)
                m8[0] = top
            for p in range(first, last):
                e = jnp.exp(z[pl.ds(p * PIECE, PIECE)].reshape(PIECE // 8, 8, tokens) - top[None])
                total = total + jnp.sum(e, axis=0)
            s8[...] = total

        def block(b, which, refill=None, drained=None, norm=False, last=False):
            for j in range(passes):
                if j % part_passes == 0:
                    ring_copy(b, j // part_passes).wait()
                    if j == 0 and refill is not None:
                        refill()
                for q in range(2):
                    if norm and j + 1 < passes:
                        normalize(2 * (j + 1) + q)
                    if not (last and j + 1 == passes):
                        push((j + 1) % passes, q)
                for q in range(2):
                    accumulate(b, j, q, which)
                if drained is not None:
                    if j in (2, 3):
                        half = n_piece // 2
                        drain(*drained, (j - 2) * half, (j - 1) * half)
                    if j in (4, 5):
                        exps((j - 4) * half, (j - 3) * half)

        def refill(b):
            def start():
                @pl.when(b - 1 + RING < n_blocks)
                def _():
                    for i in range(PARTS):
                        ring_copy(b - 1 + RING, i).start()
            return start

        for q in range(2):
            normalize(q)
            push(0, q)
        block(0, 0, norm=True)

        def two(i, carry):
            b = 2 * i + 1
            block(b, 1, refill(b), drained=(b - 1, 0))
            block(b + 1, 0, refill(b + 1), drained=(b, 1))
            return carry

        lax.fori_loop(0, (n_blocks - 3) // 2, two, 0)
        b = n_blocks - 2
        block(b, 1, drained=(b - 1, 0))
        block(b + 1, 0, drained=(b, 1), last=True)
        drain(b + 1, 0, 0, n_piece)
        exps(0, n_piece)

    pl.run_scoped(matmuls, *[pltpu.ACC(q)((PIECE, TILE), F32)
                             for _ in range(2) for q in range(2) for _ in range(BLOCK // PIECE)])

    top = jnp.max(m8[0], axis=0, keepdims=True)
    total = jnp.sum(s8[...] * jnp.exp(m8[0] - top), axis=0, keepdims=True)
    picked = jnp.sum(t8[...], axis=0, keepdims=True)
    stats_ref[...] = jnp.concatenate([top, total, picked], axis=1)


def combine_kernel(n_tp, stats_ref, mask, norm_ref, logp_ref, seq_ref, top_ref, box, send_sem, recv_sem):
    tokens = mask.shape[1]
    me = lax.axis_index("tp")

    def peer(d):
        return lax.rem(me + d, n_tp)

    def exchange(d, slot):
        return pltpu.make_async_remote_copy(
            src_ref=stats_ref, dst_ref=box.at[slot], send_sem=send_sem.at[d], recv_sem=recv_sem.at[slot],
            device_id={"tp": peer(d)}, device_id_type=pl.DeviceIdType.MESH)

    barrier = pltpu.get_barrier_semaphore()
    for d in range(1, n_tp):
        pl.semaphore_signal(barrier, inc=1, device_id={"tp": peer(d)}, device_id_type=pl.DeviceIdType.MESH)
    pl.semaphore_wait(barrier, n_tp - 1)
    for d in range(1, n_tp):
        exchange(d, me).start()
    box[me] = stats_ref[...]
    for d in range(1, n_tp):
        exchange(d, peer(d)).wait_recv()

    boxes = [box[i] for i in range(n_tp)]
    top = functools.reduce(jnp.maximum, [x[:, :tokens] for x in boxes])
    total = sum(x[:, tokens:2 * tokens] * jnp.exp(x[:, :tokens] - top) for x in boxes)
    picked = sum(x[:, 2 * tokens:] for x in boxes)
    log_norm = top + jnp.log(total)
    token_logp = (picked - log_norm) * mask[...].astype(F32)
    norm_ref[...] = log_norm
    logp_ref[...] = token_logp
    top_ref[...] = top - log_norm
    seq_ref[...] = jnp.broadcast_to(jnp.sum(token_logp, axis=-1, keepdims=True), seq_ref.shape)
    for d in range(1, n_tp):
        exchange(d, me).wait_send()


def solution(mesh):
    n_tp = mesh.shape["tp"]

    def local_part(hidden, ln_gain, ln_bias, embedding, targets, score_mask):
        prompts, tokens, width = hidden.shape
        rows = embedding.shape[0]
        assert prompts == 1 and tokens == TILE and rows % (2 * BLOCK) == BLOCK and width % (2 * TILE * PARTS) == 0
        row = jax.ShapeDtypeStruct((prompts, tokens), F32)
        stats = pl.pallas_call(
            head_kernel,
            out_shape=jax.ShapeDtypeStruct((1, 3 * tokens), F32),
            in_specs=[pl.BlockSpec(memory_space=pl.ANY)] * 5,
            out_specs=pl.BlockSpec(memory_space=pltpu.VMEM),
            scratch_shapes=[
                pltpu.VMEM((tokens, width), hidden.dtype),
                pltpu.VMEM((RING, BLOCK, width), embedding.dtype),
                pltpu.VMEM((BLOCK, tokens), F32),
                pltpu.VMEM((1, width), F32),
                pltpu.VMEM((1, width), F32),
                pltpu.VMEM((1, tokens), jnp.int32),
                pltpu.VMEM((tokens, LANES), F32),
                pltpu.VMEM((tokens, LANES), F32),
                pltpu.VMEM((tokens, LANES), F32),
                pltpu.VMEM((2, 8, tokens), F32),
                pltpu.VMEM((8, tokens), F32),
                pltpu.VMEM((8, tokens), F32),
                pltpu.SemaphoreType.DMA((3,)),
                pltpu.SemaphoreType.DMA((HID_PARTS,)),
                pltpu.SemaphoreType.DMA((RING, PARTS)),
            ],
            compiler_params=pltpu.CompilerParams(vmem_limit_bytes=67043328),
            name="head",
        )(hidden, ln_gain.reshape(1, width), ln_bias.reshape(1, width), embedding, targets)
        vmem = pl.BlockSpec(memory_space=pltpu.VMEM)
        log_norm, token_logp, seq, top_logp = pl.pallas_call(
            functools.partial(combine_kernel, n_tp),
            out_shape=(row, row, jax.ShapeDtypeStruct((prompts, LANES), F32), row),
            in_specs=[vmem] * 2,
            out_specs=[vmem] * 4,
            scratch_shapes=[
                pltpu.VMEM((n_tp, 1, 3 * tokens), F32),
                pltpu.SemaphoreType.DMA((n_tp,)),
                pltpu.SemaphoreType.DMA((n_tp,)),
            ],
            compiler_params=pltpu.CompilerParams(collective_id=0, has_side_effects=True),
            name="combine",
        )(stats, score_mask)
        return log_norm, token_logp, seq[:, 0], top_logp

    row_spec = P("dp", None)
    return jax.shard_map(local_part, mesh=mesh,
                         in_specs=(P("dp", None, None), P(), P(), P("tp", None), row_spec, row_spec),
                         out_specs=(row_spec, row_spec, P("dp"), row_spec), check_vma=False)
```

```python
import functools

import jax
import jax.numpy as jnp
from jax import lax
from jax.experimental import pallas as pl
from jax.experimental.pallas import tpu as pltpu
from jax.sharding import PartitionSpec as P

OPT_VOCAB = 50272
LN_EPS = 1e-5

TILE = 256
BLOCK = 256
PIECE = 64
LANES = 128
RING = 12
PARTS = 3
HID_PARTS = 4
F32 = jnp.float32
SMALL_VMEM = 1 << 20
HEAD_VMEM = 61 << 20


def head_kernel(hid_hbm, gain_hbm, bias_hbm, emb_hbm, tgt_hbm, stats_ref,
                h, ring, z, gain, bias, tgt, mean_b, rstd_b, part, m8, s8, t8, small_sem, hid_sem, ring_sem):
    tokens, width = h.shape
    rows = emb_hbm.shape[0]
    n_blocks = rows // BLOCK
    passes = width // (2 * TILE)
    part_width = width // PARTS
    part_passes = passes // PARTS
    hid_rows = tokens // HID_PARTS
    me = lax.axis_index("tp")
    base = me * rows

    def hid_copy(i):
        at = pl.ds(i * hid_rows, hid_rows)
        return pltpu.make_async_copy(hid_hbm.at[0, at], h.at[at], hid_sem.at[i])

    def ring_copy(b, i):
        slot = lax.rem(b, RING)
        cols = pl.ds(i * part_width, part_width)
        return pltpu.make_async_copy(
            emb_hbm.at[pl.ds(b * BLOCK, BLOCK), cols], ring.at[slot, :, cols], ring_sem.at[slot, i])

    small = [pltpu.make_async_copy(src, dst, small_sem.at[i]) for i, (src, dst) in enumerate(
        ((gain_hbm, gain), (bias_hbm, bias), (tgt_hbm, tgt)))]

    for i in range(HID_PARTS):
        hid_copy(i).start()
    for copy in small:
        copy.start()
    for b in range(min(RING, n_blocks)):
        for i in range(PARTS):
            ring_copy(b, i).start(priority=1)

    def lane_sum(r, n, fn):
        acc = [jnp.zeros((n, LANES), F32) for _ in range(2)]
        for c in range(width // LANES):
            acc[c % 2] += fn(h[pl.ds(r, n), pl.ds(c * LANES, LANES)].astype(F32))
        return acc[0] + acc[1]

    group = 16

    def mean_rows(i):
        for g in range(hid_rows // group):
            r = i * hid_rows + g * group
            part[pl.ds(r, group)] = lane_sum(r, group, lambda x: x)
        at = pl.ds(i * hid_rows, hid_rows)
        mean = jnp.sum(part[at], axis=-1, keepdims=True) * (1.0 / width)
        mean_b[at] = jnp.broadcast_to(mean, (hid_rows, LANES))

    def var_rows(i):
        for g in range(hid_rows // group):
            r = i * hid_rows + g * group
            mean = mean_b[pl.ds(r, group)]
            part[pl.ds(r, group)] = lane_sum(r, group, lambda x: (x - mean) * (x - mean))
        at = pl.ds(i * hid_rows, hid_rows)
        var = jnp.sum(part[at], axis=-1, keepdims=True) * (1.0 / width)
        rstd_b[at] = jnp.broadcast_to(lax.rsqrt(var + LN_EPS), (hid_rows, LANES))

    for i in range(HID_PARTS):
        hid_copy(i).wait()
        mean_rows(i)
        if i:
            var_rows(i - 1)
    var_rows(HID_PARTS - 1)

    for copy in small:
        copy.wait()
    m8[...] = jnp.full_like(m8, jnp.finfo(F32).min)
    s8[...] = jnp.zeros_like(s8)
    t8[...] = jnp.zeros_like(t8)

    def normalize(k):
        for c in range(TILE // LANES):
            cols = pl.ds(k * TILE + c * LANES, LANES)
            x = h[:, cols].astype(F32)
            x = (x - mean_b[...]) * rstd_b[...] * gain[:, cols] + bias[:, cols]
            h[:, cols] = x.astype(h.dtype)

    def matmuls(*accs):
        n_piece = BLOCK // PIECE
        accs = [[list(accs[(w * 2 + q) * n_piece:(w * 2 + q + 1) * n_piece]) for q in range(2)] for w in range(2)]

        for which in accs:
            for q in which:
                for acc in q:
                    z[pl.ds(0, PIECE)] = pltpu.matmul_pop(acc)

        def push(j, q):
            k = 2 * j + q
            pltpu.matmul_push_rhs(h[:, pl.ds(k * TILE, TILE)], staging_register=j % 2, mxu_index=q, transpose=True)

        def accumulate(b, j, q, which):
            slot = lax.rem(b, RING)
            cols = pl.ds((2 * j + q) * TILE, TILE)
            for p in range(n_piece):
                lhs = ring[slot, pl.ds(p * PIECE, PIECE), cols]
                pltpu.matmul_acc_lhs(accs[which][q][p], lhs, load_staged_rhs=j % 2 if p == 0 else None)

        def drain(b, which, first, last):
            offset = base + b * BLOCK
            target = tgt[...] - offset
            limit = OPT_VOCAB - offset
            top, picked = m8[1], t8[...]
            for p in range(first, last):
                logits = pltpu.matmul_pop(accs[which][0][p]) + pltpu.matmul_pop(accs[which][1][p])
                row = lax.broadcasted_iota(jnp.int32, logits.shape, 0) + p * PIECE
                logits = jnp.where(row < limit, logits, -jnp.inf)
                z[pl.ds(p * PIECE, PIECE)] = logits
                top = jnp.maximum(top, jnp.max(logits.reshape(PIECE // 8, 8, tokens), axis=0))
                hit = jnp.where(row == target, logits, 0.0)
                picked = picked + jnp.sum(hit.reshape(PIECE // 8, 8, tokens), axis=0)
            m8[1] = top
            t8[...] = picked

        def exps(first, last):
            top = m8[1]
            total = s8[...]
            if first == 0:
                total = total * jnp.exp(m8[0] - top)
                m8[0] = top
            for p in range(first, last):
                e = jnp.exp(z[pl.ds(p * PIECE, PIECE)].reshape(PIECE // 8, 8, tokens) - top[None])
                total = total + jnp.sum(e, axis=0)
            s8[...] = total

        def block(b, which, refill=None, drained=None, norm=False, last=False):
            for j in range(passes):
                if j % part_passes == 0:
                    ring_copy(b, j // part_passes).wait()
                    if j == 0 and refill is not None:
                        refill()
                for q in range(2):
                    if norm and j + 1 < passes:
                        normalize(2 * (j + 1) + q)
                    if not (last and j + 1 == passes):
                        push((j + 1) % passes, q)
                for q in range(2):
                    accumulate(b, j, q, which)
                if drained is not None:
                    if j in (2, 3):
                        half = n_piece // 2
                        drain(*drained, (j - 2) * half, (j - 1) * half)
                    if j in (4, 5):
                        exps((j - 4) * half, (j - 3) * half)

        def refill(b):
            def start():
                @pl.when(b - 1 + RING < n_blocks)
                def _():
                    for i in range(PARTS):
                        ring_copy(b - 1 + RING, i).start(priority=1)
            return start

        for q in range(2):
            normalize(q)
            push(0, q)
        block(0, 0, norm=True)

        def two(i, carry):
            b = 2 * i + 1
            block(b, 1, refill(b), drained=(b - 1, 0))
            block(b + 1, 0, refill(b + 1), drained=(b, 1))
            return carry

        lax.fori_loop(0, (n_blocks - 3) // 2, two, 0)
        b = n_blocks - 2
        block(b, 1, drained=(b - 1, 0))
        block(b + 1, 0, drained=(b, 1), last=True)
        drain(b + 1, 0, 0, n_piece)
        exps(0, n_piece)

    pl.run_scoped(matmuls, *[pltpu.ACC(q)((PIECE, TILE), F32)
                             for _ in range(2) for q in range(2) for _ in range(BLOCK // PIECE)])

    top = jnp.max(m8[0], axis=0, keepdims=True)
    total = jnp.sum(s8[...] * jnp.exp(m8[0] - top), axis=0, keepdims=True)
    picked = jnp.sum(t8[...], axis=0, keepdims=True)
    stats_ref[...] = jnp.concatenate([top, total, picked], axis=1)


def exchange_kernel(n_tp, stats_ref, out_ref, box, send_sem, recv_sem):
    me = lax.axis_index("tp")

    def peer(d):
        return lax.rem(me + d, n_tp)

    def exchange(d, slot):
        return pltpu.make_async_remote_copy(
            src_ref=stats_ref, dst_ref=box.at[slot], send_sem=send_sem.at[d], recv_sem=recv_sem.at[slot],
            device_id={"tp": peer(d)}, device_id_type=pl.DeviceIdType.MESH)

    barrier = pltpu.get_barrier_semaphore()
    for d in range(1, n_tp):
        pl.semaphore_signal(barrier, inc=1, device_id={"tp": peer(d)}, device_id_type=pl.DeviceIdType.MESH)
    pl.semaphore_wait(barrier, n_tp - 1)
    for d in range(1, n_tp):
        exchange(d, me).start()
    box[me] = stats_ref[...]
    for d in range(1, n_tp):
        exchange(d, peer(d)).wait_recv()
    out_ref[...] = box[...]
    for d in range(1, n_tp):
        exchange(d, me).wait_send()


def finish_kernel(box, mask, norm_ref, logp_ref, seq_ref, top_ref):
    n_tp, _, width = box.shape
    tokens = width // 3
    boxes = [box[i] for i in range(n_tp)]
    top = functools.reduce(jnp.maximum, [x[:, :tokens] for x in boxes])
    total = sum(x[:, tokens:2 * tokens] * jnp.exp(x[:, :tokens] - top) for x in boxes)
    picked = sum(x[:, 2 * tokens:] for x in boxes)
    log_norm = top + jnp.log(total)
    token_logp = (picked - log_norm) * mask[...].astype(F32)
    norm_ref[...] = log_norm
    logp_ref[...] = token_logp
    top_ref[...] = top - log_norm
    seq_ref[...] = jnp.broadcast_to(jnp.sum(token_logp, axis=-1, keepdims=True), seq_ref.shape)


def solution(mesh):
    n_tp = mesh.shape["tp"]

    def local_part(hidden, ln_gain, ln_bias, embedding, targets, score_mask):
        prompts, tokens, width = hidden.shape
        rows = embedding.shape[0]
        assert prompts == 1 and tokens == TILE and rows % (2 * BLOCK) == BLOCK and width % (2 * TILE * PARTS) == 0
        row = jax.ShapeDtypeStruct((prompts, tokens), F32)
        stats = pl.pallas_call(
            head_kernel,
            out_shape=jax.ShapeDtypeStruct((1, 3 * tokens), F32),
            in_specs=[pl.BlockSpec(memory_space=pl.ANY)] * 5,
            out_specs=pl.BlockSpec(memory_space=pltpu.VMEM),
            scratch_shapes=[
                pltpu.VMEM((tokens, width), hidden.dtype),
                pltpu.VMEM((RING, BLOCK, width), embedding.dtype),
                pltpu.VMEM((BLOCK, tokens), F32),
                pltpu.VMEM((1, width), F32),
                pltpu.VMEM((1, width), F32),
                pltpu.VMEM((1, tokens), jnp.int32),
                pltpu.VMEM((tokens, LANES), F32),
                pltpu.VMEM((tokens, LANES), F32),
                pltpu.VMEM((tokens, LANES), F32),
                pltpu.VMEM((2, 8, tokens), F32),
                pltpu.VMEM((8, tokens), F32),
                pltpu.VMEM((8, tokens), F32),
                pltpu.SemaphoreType.DMA((3,)),
                pltpu.SemaphoreType.DMA((HID_PARTS,)),
                pltpu.SemaphoreType.DMA((RING, PARTS)),
            ],
            compiler_params=pltpu.CompilerParams(vmem_limit_bytes=HEAD_VMEM),
            name="head",
        )(hidden, ln_gain.reshape(1, width), ln_bias.reshape(1, width), embedding, targets)
        vmem = pl.BlockSpec(memory_space=pltpu.VMEM)
        boxes = pl.pallas_call(
            functools.partial(exchange_kernel, n_tp),
            out_shape=jax.ShapeDtypeStruct((n_tp, 1, 3 * tokens), F32),
            in_specs=[vmem],
            out_specs=vmem,
            scratch_shapes=[
                pltpu.VMEM((n_tp, 1, 3 * tokens), F32),
                pltpu.SemaphoreType.DMA((n_tp,)),
                pltpu.SemaphoreType.DMA((n_tp,)),
            ],
            compiler_params=pltpu.CompilerParams(
                collective_id=0, has_side_effects=True, vmem_limit_bytes=SMALL_VMEM),
            name="exchange",
        )(stats)
        log_norm, token_logp, seq, top_logp = pl.pallas_call(
            finish_kernel,
            out_shape=(row, row, jax.ShapeDtypeStruct((prompts, LANES), F32), row),
            in_specs=[vmem] * 2,
            out_specs=[vmem] * 4,
            compiler_params=pltpu.CompilerParams(vmem_limit_bytes=SMALL_VMEM),
            name="finish",
        )(boxes, score_mask)
        return log_norm, token_logp, seq[:, 0], top_logp

    row_spec = P("dp", None)
    return jax.shard_map(local_part, mesh=mesh,
                         in_specs=(P("dp", None, None), P(), P(), P("tp", None), row_spec, row_spec),
                         out_specs=(row_spec, row_spec, P("dp"), row_spec), check_vma=False)
```

```python
import functools

import jax
import jax.numpy as jnp
from jax import lax
from jax.experimental import pallas as pl
from jax.experimental.pallas import tpu as pltpu
from jax.sharding import PartitionSpec as P

OPT_VOCAB = 50272
LN_EPS = 1e-5

TILE = 256
CHUNK = 256
PIECE = 64
LANES = 128
RING = 10
FIRST = 3
PARTS = 6
HID_PARTS = 4
NORM_ROWS = 32
HEAD_VMEM = 52 << 20
SMALL_VMEM = 1 << 20
F32 = jnp.float32


def head_kernel(hid_hbm, gain_hbm, bias_hbm, emb_hbm, tgt_hbm, stats_ref,
                h, ring, z, gain, bias, tgt, mean_b, rstd_b, part, m8, s8, t8, small_sem, hid_sem, ring_sem,
                first_sem, last_sem):
    tokens, width = h.shape
    rows = emb_hbm.shape[0]
    n_chunks = rows // CHUNK
    passes = width // (2 * TILE)
    part_width = width // PARTS
    part_passes = passes // PARTS
    hid_rows = tokens // HID_PARTS
    base = lax.axis_index("tp") * rows

    def hid_copy(i):
        at = pl.ds(i * hid_rows, hid_rows)
        return pltpu.make_async_copy(hid_hbm.at[0, at], h.at[at], hid_sem.at[i])

    def chunk_copy(c):
        slot = lax.rem(c, RING)
        return pltpu.make_async_copy(emb_hbm.at[pl.ds(c * CHUNK, CHUNK)], ring.at[slot], ring_sem.at[slot])

    def part_copy(c, i, sem):
        cols = pl.ds(i * part_width, part_width)
        return pltpu.make_async_copy(
            emb_hbm.at[pl.ds(c * CHUNK, CHUNK), cols], ring.at[lax.rem(c, RING), :, cols], sem)

    def first_copy(e, i):
        return part_copy(e, i, first_sem.at[e, i])

    def last_copy(e, i):
        return part_copy(n_chunks - 2 + e, i, last_sem.at[e, i])

    small = [pltpu.make_async_copy(src, dst, small_sem.at[i]) for i, (src, dst) in enumerate(
        ((gain_hbm, gain), (bias_hbm, bias), (tgt_hbm, tgt)))]

    for i in range(HID_PARTS):
        hid_copy(i).start()
    for copy in small:
        copy.start()
    for i in range(PARTS):
        for e in range(FIRST):
            first_copy(e, i).start(priority=1)
    for c in range(FIRST, RING):
        chunk_copy(c).start(priority=1)

    def lane_sum(r, n, fn):
        acc = [jnp.zeros((n, LANES), F32) for _ in range(2)]
        for c in range(width // LANES):
            acc[c % 2] += fn(h[pl.ds(r, n), pl.ds(c * LANES, LANES)].astype(F32))
        return acc[0] + acc[1]

    group = 16

    def mean_rows(i):
        for g in range(hid_rows // group):
            r = i * hid_rows + g * group
            part[pl.ds(r, group)] = lane_sum(r, group, lambda x: x)
        at = pl.ds(i * hid_rows, hid_rows)
        mean = jnp.sum(part[at], axis=-1, keepdims=True) * (1.0 / width)
        mean_b[at] = jnp.broadcast_to(mean, (hid_rows, LANES))

    def var_rows(i):
        for g in range(hid_rows // group):
            r = i * hid_rows + g * group
            mean = mean_b[pl.ds(r, group)]
            part[pl.ds(r, group)] = lane_sum(r, group, lambda x: (x - mean) * (x - mean))
        at = pl.ds(i * hid_rows, hid_rows)
        var = jnp.sum(part[at], axis=-1, keepdims=True) * (1.0 / width)
        rstd_b[at] = jnp.broadcast_to(lax.rsqrt(var + LN_EPS), (hid_rows, LANES))

    for i in range(HID_PARTS):
        hid_copy(i).wait()
        mean_rows(i)
        if i:
            var_rows(i - 1)
    var_rows(HID_PARTS - 1)

    for copy in small:
        copy.wait()
    m8[...] = jnp.full_like(m8, jnp.finfo(F32).min)
    s8[...] = jnp.zeros_like(s8)
    t8[...] = jnp.zeros_like(t8)

    def normalize(k, r=0, n=tokens):
        at, cols = pl.ds(r, n), pl.ds(k * TILE, TILE)
        wide = lambda x: jnp.concatenate([x] * (TILE // LANES), axis=1)
        x = h[at, cols].astype(F32)
        x = (x - wide(mean_b[at])) * wide(rstd_b[at]) * gain[:, cols] + bias[:, cols]
        h[at, cols] = x.astype(h.dtype)

    def matmuls(*accs):
        n_piece = CHUNK // PIECE
        accs = [[accs[(w * 2 + q) * n_piece:(w * 2 + q + 1) * n_piece] for q in range(2)] for w in range(4)]

        for which in accs:
            for q in which:
                for acc in q:
                    z[pl.ds(0, PIECE)] = pltpu.matmul_pop(acc)

        def push(j, q):
            cols = pl.ds((2 * j + q) * TILE, TILE)
            pltpu.matmul_push_rhs(h[:, cols], staging_register=j % 2, mxu_index=q, transpose=True)

        def accumulate(chunks, sets, j):
            def step(c, which, p, q):
                lhs = ring[lax.rem(c, RING), pl.ds(p * PIECE, PIECE), pl.ds((2 * j + q) * TILE, TILE)]
                pltpu.matmul_acc_lhs(
                    accs[which][q][p], lhs, load_staged_rhs=j % 2 if which == sets[0] and p == 0 else None)
            return [functools.partial(step, c, which, p, q)
                    for c, which in zip(chunks, sets) for p in range(n_piece) for q in range(2)]

        def drain(c, which, p):
            offset = base + c * CHUNK
            target = tgt[...] - offset
            limit = OPT_VOCAB - offset
            shape = (PIECE // 8, 8, tokens)
            logits = pltpu.matmul_pop(accs[which][0][p]) + pltpu.matmul_pop(accs[which][1][p])
            row = lax.broadcasted_iota(jnp.int32, logits.shape, 0) + p * PIECE
            logits = jnp.where(row < limit, logits, -jnp.inf)
            z[pl.ds(p * PIECE, PIECE)] = logits
            m8[1] = jnp.maximum(m8[1], jnp.max(logits.reshape(shape), axis=0))
            t8[...] += jnp.sum(jnp.where(row == target, logits, 0.0).reshape(shape), axis=0)

        def exps(p):
            top = m8[1]
            total = s8[...]
            if p == 0:
                total = total * jnp.exp(m8[0] - top)
                m8[0] = top
            e = jnp.exp(z[pl.ds(p * PIECE, PIECE)].reshape(PIECE // 8, 8, tokens) - top[None])
            s8[...] = total + jnp.sum(e, axis=0)

        def absorb(c, which):
            return [functools.partial(drain, c, which, p) for p in range(n_piece)] + [
                functools.partial(exps, p) for p in range(n_piece)]

        def sweep(chunks, sets, beside=(), wait=None, norm=False, last=False):
            beside = list(beside)
            per_pass = pl.cdiv(len(beside), passes - 3)
            for j in range(passes):
                if wait is not None and j % part_passes == 0:
                    wait(j // part_passes)
                def push_next():
                    for q in range(2):
                        if not (last and j + 1 == passes):
                            push((j + 1) % passes, q)

                steps = accumulate(chunks, sets, j)
                if norm and j + 1 < passes:
                    cut = len(steps) * 2 // 3
                    groups = [(2 * (j + 1) + q, r) for q in range(2) for r in range(0, tokens, NORM_ROWS)]
                    for i, step in enumerate(steps):
                        for k, r in groups[i * len(groups) // cut:(i + 1) * len(groups) // cut]:
                            normalize(k, r, NORM_ROWS)
                        if i == cut:
                            push_next()
                        step()
                else:
                    push_next()
                    for step in steps:
                        step()
                if j >= 2:
                    for step in beside[(j - 2) * per_pass:(j - 1) * per_pass]:
                        step()

        def first_wait(i):
            for e in range(FIRST):
                first_copy(e, i).wait()

        def last_wait(i):
            for e in range(2):
                last_copy(e, i).wait()

        for k in range(2):
            normalize(k)
        for q in range(2):
            push(0, q)
        sweep(range(FIRST), range(FIRST), wait=first_wait, norm=True)
        for step in absorb(0, 0):
            step()
        for c in range(RING, RING + FIRST - 2):
            chunk_copy(c).start(priority=1)

        def pair(c, sets, old, refill=True):
            for e in range(2):
                chunk_copy(c + e).wait()
            if refill:
                @pl.when(c + RING < n_chunks)
                def _():
                    for e in range(2):
                        chunk_copy(c - 2 + e + RING).start(priority=1)

                @pl.when(c + RING == n_chunks)
                def _():
                    for i in range(PARTS):
                        for e in range(2):
                            last_copy(e, i).start(priority=1)
            sweep((c, c + 1), sets, absorb(c - 2, old[0]) + absorb(c - 1, old[1]))

        def two_pairs(i, carry):
            c = FIRST + 4 * i
            pair(c, (3, 0), (1, 2))
            pair(c + 2, (1, 2), (3, 0))
            return carry

        lax.fori_loop(0, (n_chunks - FIRST) // 4, two_pairs, 0)
        c = n_chunks - 2
        sweep((c, c + 1), (3, 0), absorb(c - 2, 1) + absorb(c - 1, 2), wait=last_wait, last=True)
        for step in absorb(c, 3) + absorb(c + 1, 0):
            step()

    pl.run_scoped(matmuls, *[pltpu.ACC(q)((PIECE, TILE), F32)
                             for _ in range(4) for q in range(2) for _ in range(CHUNK // PIECE)])

    top = jnp.max(m8[0], axis=0, keepdims=True)
    total = jnp.sum(s8[...] * jnp.exp(m8[0] - top), axis=0, keepdims=True)
    picked = jnp.sum(t8[...], axis=0, keepdims=True)
    stats_ref[...] = jnp.concatenate([top, total, picked], axis=1)


def exchange_kernel(n_tp, stats_ref, out_ref, box, send_sem, recv_sem):
    me = lax.axis_index("tp")

    def peer(d):
        return lax.rem(me + d, n_tp)

    def exchange(d, slot):
        return pltpu.make_async_remote_copy(
            src_ref=stats_ref, dst_ref=box.at[slot], send_sem=send_sem.at[d], recv_sem=recv_sem.at[slot],
            device_id={"tp": peer(d)}, device_id_type=pl.DeviceIdType.MESH)

    barrier = pltpu.get_barrier_semaphore()
    for d in range(1, n_tp):
        pl.semaphore_signal(barrier, inc=1, device_id={"tp": peer(d)}, device_id_type=pl.DeviceIdType.MESH)
    pl.semaphore_wait(barrier, n_tp - 1)
    for d in range(1, n_tp):
        exchange(d, me).start()
    box[me] = stats_ref[...]
    for d in range(1, n_tp):
        exchange(d, peer(d)).wait_recv()
    out_ref[...] = box[...]
    for d in range(1, n_tp):
        exchange(d, me).wait_send()


def finish_kernel(box, mask, norm_ref, logp_ref, seq_ref, top_ref):
    n_tp, _, width = box.shape
    tokens = width // 3
    boxes = [box[i] for i in range(n_tp)]
    top = functools.reduce(jnp.maximum, [x[:, :tokens] for x in boxes])
    total = sum(x[:, tokens:2 * tokens] * jnp.exp(x[:, :tokens] - top) for x in boxes)
    picked = sum(x[:, 2 * tokens:] for x in boxes)
    log_norm = top + jnp.log(total)
    token_logp = (picked - log_norm) * mask[...].astype(F32)
    norm_ref[...] = log_norm
    logp_ref[...] = token_logp
    top_ref[...] = top - log_norm
    seq_ref[...] = jnp.broadcast_to(jnp.sum(token_logp, axis=-1, keepdims=True), seq_ref.shape)


def solution(mesh):
    n_tp = mesh.shape["tp"]

    def local_part(hidden, ln_gain, ln_bias, embedding, targets, score_mask):
        prompts, tokens, width = hidden.shape
        rows = embedding.shape[0]
        n_chunks = rows // CHUNK
        assert prompts == 1 and tokens == TILE and rows % CHUNK == 0 and width % (2 * TILE * PARTS) == 0
        assert (n_chunks - FIRST) % 4 == 2 and n_chunks > RING + FIRST + 2
        row = jax.ShapeDtypeStruct((prompts, tokens), F32)
        stats = pl.pallas_call(
            head_kernel,
            out_shape=jax.ShapeDtypeStruct((1, 3 * tokens), F32),
            in_specs=[pl.BlockSpec(memory_space=pl.ANY)] * 5,
            out_specs=pl.BlockSpec(memory_space=pltpu.VMEM),
            scratch_shapes=[
                pltpu.VMEM((tokens, width), hidden.dtype),
                pltpu.VMEM((RING, CHUNK, width), embedding.dtype),
                pltpu.VMEM((CHUNK, tokens), F32),
                pltpu.VMEM((1, width), F32),
                pltpu.VMEM((1, width), F32),
                pltpu.VMEM((1, tokens), jnp.int32),
                pltpu.VMEM((tokens, LANES), F32),
                pltpu.VMEM((tokens, LANES), F32),
                pltpu.VMEM((tokens, LANES), F32),
                pltpu.VMEM((2, 8, tokens), F32),
                pltpu.VMEM((8, tokens), F32),
                pltpu.VMEM((8, tokens), F32),
                pltpu.SemaphoreType.DMA((3,)),
                pltpu.SemaphoreType.DMA((HID_PARTS,)),
                pltpu.SemaphoreType.DMA((RING,)),
                pltpu.SemaphoreType.DMA((FIRST, PARTS)),
                pltpu.SemaphoreType.DMA((2, PARTS)),
            ],
            compiler_params=pltpu.CompilerParams(vmem_limit_bytes=HEAD_VMEM),
            name="head",
        )(*[pltpu.with_memory_space_constraint(x, pltpu.HBM) for x in (
            hidden, ln_gain.reshape(1, width), ln_bias.reshape(1, width), embedding, targets)])
        vmem = pl.BlockSpec(memory_space=pltpu.VMEM)
        boxes = pl.pallas_call(
            functools.partial(exchange_kernel, n_tp),
            out_shape=jax.ShapeDtypeStruct((n_tp, 1, 3 * tokens), F32),
            in_specs=[vmem],
            out_specs=vmem,
            scratch_shapes=[
                pltpu.VMEM((n_tp, 1, 3 * tokens), F32),
                pltpu.SemaphoreType.DMA((n_tp,)),
                pltpu.SemaphoreType.DMA((n_tp,)),
            ],
            compiler_params=pltpu.CompilerParams(
                collective_id=0, has_side_effects=True, vmem_limit_bytes=SMALL_VMEM),
            name="exchange",
        )(stats)
        log_norm, token_logp, seq, top_logp = pl.pallas_call(
            finish_kernel,
            out_shape=(row, row, jax.ShapeDtypeStruct((prompts, LANES), F32), row),
            in_specs=[vmem] * 2,
            out_specs=[vmem] * 4,
            compiler_params=pltpu.CompilerParams(vmem_limit_bytes=SMALL_VMEM),
            name="finish",
        )(boxes, score_mask)
        return log_norm, token_logp, seq[:, 0], top_logp

    row_spec = P("dp", None)
    return jax.shard_map(local_part, mesh=mesh,
                         in_specs=(P("dp", None, None), P(), P(), P("tp", None), row_spec, row_spec),
                         out_specs=(row_spec, row_spec, P("dp"), row_spec), check_vma=False)
```

```python
import functools

import jax
import jax.numpy as jnp
from jax import lax
from jax.experimental import pallas as pl
from jax.experimental.pallas import tpu as pltpu
from jax.sharding import PartitionSpec as P

OPT_VOCAB = 50272
LN_EPS = 1e-5

TILE = 256
CHUNK = 256
PIECE = 64
LANES = 128
RING = 8
FIRST = 3
PARTS = 6
HID_PARTS = 4
NORM_ROWS = 32
HEAD_VMEM = 52 << 20
SMALL_VMEM = 1 << 20
F32 = jnp.float32


def head_kernel(hid_hbm, gain_hbm, bias_hbm, emb_hbm, tgt_hbm, stats_ref,
                h, ring, z, gain, bias, tgt, mean_b, rstd_b, part, m8, s8, t8, small_sem, hid_sem, ring_sem,
                first_sem, last_sem):
    tokens, width = h.shape
    rows = emb_hbm.shape[0]
    n_chunks = rows // CHUNK
    passes = width // (2 * TILE)
    part_width = width // PARTS
    part_passes = passes // PARTS
    hid_rows = tokens // HID_PARTS
    base = lax.axis_index("tp") * rows

    def hid_copy(i):
        at = pl.ds(i * hid_rows, hid_rows)
        return pltpu.make_async_copy(hid_hbm.at[0, at], h.at[at], hid_sem.at[i])

    def chunk_copy(c):
        slot = lax.rem(c, RING)
        return pltpu.make_async_copy(emb_hbm.at[pl.ds(c * CHUNK, CHUNK)], ring.at[slot], ring_sem.at[slot])

    def part_copy(c, i, sem):
        cols = pl.ds(i * part_width, part_width)
        return pltpu.make_async_copy(
            emb_hbm.at[pl.ds(c * CHUNK, CHUNK), cols], ring.at[lax.rem(c, RING), :, cols], sem)

    def first_copy(e, i):
        return part_copy(e, i, first_sem.at[e, i])

    def last_copy(e, i):
        return part_copy(n_chunks - 2 + e, i, last_sem.at[e, i])

    small = [pltpu.make_async_copy(src, dst, small_sem.at[i]) for i, (src, dst) in enumerate(
        ((gain_hbm, gain), (bias_hbm, bias), (tgt_hbm, tgt)))]

    for i in range(HID_PARTS):
        hid_copy(i).start()
    for copy in small:
        copy.start()
    early = list(range(FIRST, RING))

    def lane_sum(r, n, fn):
        acc = [jnp.zeros((n, LANES), F32) for _ in range(2)]
        for c in range(width // LANES):
            acc[c % 2] += fn(h[pl.ds(r, n), pl.ds(c * LANES, LANES)].astype(F32))
        return acc[0] + acc[1]

    group = 16

    def mean_rows(i):
        for g in range(hid_rows // group):
            r = i * hid_rows + g * group
            part[pl.ds(r, group)] = lane_sum(r, group, lambda x: x)
        at = pl.ds(i * hid_rows, hid_rows)
        mean = jnp.sum(part[at], axis=-1, keepdims=True) * (1.0 / width)
        mean_b[at] = jnp.broadcast_to(mean, (hid_rows, LANES))

    def var_rows(i):
        for g in range(hid_rows // group):
            r = i * hid_rows + g * group
            mean = mean_b[pl.ds(r, group)]
            part[pl.ds(r, group)] = lane_sum(r, group, lambda x: (x - mean) * (x - mean))
        at = pl.ds(i * hid_rows, hid_rows)
        var = jnp.sum(part[at], axis=-1, keepdims=True) * (1.0 / width)
        rstd_b[at] = jnp.broadcast_to(lax.rsqrt(var + LN_EPS), (hid_rows, LANES))

    for i in range(HID_PARTS):
        hid_copy(i).wait()
        if i == 0:
            for k in range(PARTS):
                for e in range(FIRST):
                    first_copy(e, k).start(priority=1)
        mean_rows(i)
        if i:
            var_rows(i - 1)
    chunk_copy(early.pop(0)).start(priority=1)
    var_rows(HID_PARTS - 1)

    for copy in small:
        copy.wait()
    m8[...] = jnp.full_like(m8, jnp.finfo(F32).min)
    s8[...] = jnp.zeros_like(s8)
    t8[...] = jnp.zeros_like(t8)

    def normalize(k, r=0, n=tokens):
        at, cols = pl.ds(r, n), pl.ds(k * TILE, TILE)
        wide = lambda x: jnp.concatenate([x] * (TILE // LANES), axis=1)
        x = h[at, cols].astype(F32)
        x = (x - wide(mean_b[at])) * wide(rstd_b[at]) * gain[:, cols] + bias[:, cols]
        h[at, cols] = x.astype(h.dtype)

    def matmuls(*accs):
        n_piece = CHUNK // PIECE
        accs = [[accs[(w * 2 + q) * n_piece:(w * 2 + q + 1) * n_piece] for q in range(2)] for w in range(4)]

        for which in accs:
            for q in which:
                for acc in q:
                    z[pl.ds(0, PIECE)] = pltpu.matmul_pop(acc)

        def push(j, q):
            cols = pl.ds((2 * j + q) * TILE, TILE)
            pltpu.matmul_push_rhs(h[:, cols], staging_register=j % 2, mxu_index=q, transpose=True)

        def accumulate(chunks, sets, j):
            def step(c, which, p, q):
                lhs = ring[lax.rem(c, RING), pl.ds(p * PIECE, PIECE), pl.ds((2 * j + q) * TILE, TILE)]
                pltpu.matmul_acc_lhs(
                    accs[which][q][p], lhs, load_staged_rhs=j % 2 if which == sets[0] and p == 0 else None)
            return [functools.partial(step, c, which, p, q)
                    for c, which in zip(chunks, sets) for p in range(n_piece) for q in range(2)]

        def drain(c, which, p):
            offset = base + c * CHUNK
            target = tgt[...] - offset
            limit = OPT_VOCAB - offset
            shape = (PIECE // 8, 8, tokens)
            logits = pltpu.matmul_pop(accs[which][0][p]) + pltpu.matmul_pop(accs[which][1][p])
            row = lax.broadcasted_iota(jnp.int32, logits.shape, 0) + p * PIECE
            logits = jnp.where(row < limit, logits, -jnp.inf)
            z[pl.ds(p * PIECE, PIECE)] = logits
            m8[1] = jnp.maximum(m8[1], jnp.max(logits.reshape(shape), axis=0))
            t8[...] += jnp.sum(jnp.where(row == target, logits, 0.0).reshape(shape), axis=0)

        def exps(p):
            top = m8[1]
            total = s8[...]
            if p == 0:
                total = total * jnp.exp(m8[0] - top)
                m8[0] = top
            e = jnp.exp(z[pl.ds(p * PIECE, PIECE)].reshape(PIECE // 8, 8, tokens) - top[None])
            s8[...] = total + jnp.sum(e, axis=0)

        def absorb(c, which):
            return [functools.partial(drain, c, which, p) for p in range(n_piece)] + [
                functools.partial(exps, p) for p in range(n_piece)]

        def sweep(chunks, sets, beside=(), wait=None, norm=False, last=False):
            beside = list(beside)
            per_pass = pl.cdiv(len(beside), passes - 3)
            for j in range(passes):
                if wait is not None and j % part_passes == 0:
                    wait(j // part_passes)
                def push_next():
                    for q in range(2):
                        if not (last and j + 1 == passes):
                            push((j + 1) % passes, q)

                steps = accumulate(chunks, sets, j)
                if norm and j + 1 < passes:
                    cut = len(steps) * 2 // 3
                    groups = [(2 * (j + 1) + q, r) for q in range(2) for r in range(0, tokens, NORM_ROWS)]
                    for i, step in enumerate(steps):
                        for k, r in groups[i * len(groups) // cut:(i + 1) * len(groups) // cut]:
                            normalize(k, r, NORM_ROWS)
                        if i == cut:
                            push_next()
                        step()
                else:
                    push_next()
                    for step in steps:
                        step()
                if j >= 2:
                    for step in beside[(j - 2) * per_pass:(j - 1) * per_pass]:
                        step()

        def first_wait(i):
            for e in range(FIRST):
                first_copy(e, i).wait()
            for _ in range(len(early) - (PARTS - 1 - i) * len(early) // (PARTS - i)):
                chunk_copy(early.pop(0)).start(priority=1)

        def last_wait(i):
            for e in range(2):
                last_copy(e, i).wait()

        for k in range(2):
            normalize(k)
        for q in range(2):
            push(0, q)
        sweep(range(FIRST), range(FIRST), wait=first_wait, norm=True)
        for step in absorb(0, 0):
            step()
        for c in range(RING, RING + FIRST - 2):
            chunk_copy(c).start(priority=1)

        def pair(c, sets, old, refill=True):
            for e in range(2):
                chunk_copy(c + e).wait()
            if refill:
                @pl.when(c + RING < n_chunks)
                def _():
                    for e in range(2):
                        chunk_copy(c - 2 + e + RING).start(priority=1)

                @pl.when(c + RING == n_chunks)
                def _():
                    for i in range(PARTS):
                        for e in range(2):
                            last_copy(e, i).start(priority=1)
            sweep((c, c + 1), sets, absorb(c - 2, old[0]) + absorb(c - 1, old[1]))

        def two_pairs(i, carry):
            c = FIRST + 4 * i
            pair(c, (3, 0), (1, 2))
            pair(c + 2, (1, 2), (3, 0))
            return carry

        lax.fori_loop(0, (n_chunks - FIRST) // 4, two_pairs, 0)
        c = n_chunks - 2
        sweep((c, c + 1), (3, 0), absorb(c - 2, 1) + absorb(c - 1, 2), wait=last_wait, last=True)
        for step in absorb(c, 3) + absorb(c + 1, 0):
            step()

    pl.run_scoped(matmuls, *[pltpu.ACC(q)((PIECE, TILE), F32)
                             for _ in range(4) for q in range(2) for _ in range(CHUNK // PIECE)])

    top = jnp.max(m8[0], axis=0, keepdims=True)
    total = jnp.sum(s8[...] * jnp.exp(m8[0] - top), axis=0, keepdims=True)
    picked = jnp.sum(t8[...], axis=0, keepdims=True)
    stats_ref[...] = jnp.concatenate([top, total, picked], axis=1)


def exchange_kernel(n_tp, stats_ref, out_ref, box, send_sem, recv_sem):
    me = lax.axis_index("tp")

    def peer(d):
        return lax.rem(me + d, n_tp)

    def exchange(d, slot):
        return pltpu.make_async_remote_copy(
            src_ref=stats_ref, dst_ref=box.at[slot], send_sem=send_sem.at[d], recv_sem=recv_sem.at[slot],
            device_id={"tp": peer(d)}, device_id_type=pl.DeviceIdType.MESH)

    barrier = pltpu.get_barrier_semaphore()
    for d in range(1, n_tp):
        pl.semaphore_signal(barrier, inc=1, device_id={"tp": peer(d)}, device_id_type=pl.DeviceIdType.MESH)
    pl.semaphore_wait(barrier, n_tp - 1)
    for d in range(1, n_tp):
        exchange(d, me).start()
    box[me] = stats_ref[...]
    for d in range(1, n_tp):
        exchange(d, peer(d)).wait_recv()
    out_ref[...] = box[...]
    for d in range(1, n_tp):
        exchange(d, me).wait_send()


def finish_kernel(box, mask, norm_ref, logp_ref, seq_ref, top_ref):
    n_tp, _, width = box.shape
    tokens = width // 3
    boxes = [box[i] for i in range(n_tp)]
    top = functools.reduce(jnp.maximum, [x[:, :tokens] for x in boxes])
    total = sum(x[:, tokens:2 * tokens] * jnp.exp(x[:, :tokens] - top) for x in boxes)
    picked = sum(x[:, 2 * tokens:] for x in boxes)
    log_norm = top + jnp.log(total)
    token_logp = (picked - log_norm) * mask[...].astype(F32)
    norm_ref[...] = log_norm
    logp_ref[...] = token_logp
    top_ref[...] = top - log_norm
    seq_ref[...] = jnp.broadcast_to(jnp.sum(token_logp, axis=-1, keepdims=True), seq_ref.shape)


def solution(mesh):
    n_tp = mesh.shape["tp"]

    def local_part(hidden, ln_gain, ln_bias, embedding, targets, score_mask):
        prompts, tokens, width = hidden.shape
        rows = embedding.shape[0]
        n_chunks = rows // CHUNK
        assert prompts == 1 and tokens == TILE and rows % CHUNK == 0 and width % (2 * TILE * PARTS) == 0
        assert (n_chunks - FIRST) % 4 == 2 and n_chunks > RING + FIRST + 2
        row = jax.ShapeDtypeStruct((prompts, tokens), F32)
        stats = pl.pallas_call(
            head_kernel,
            out_shape=jax.ShapeDtypeStruct((1, 3 * tokens), F32),
            in_specs=[pl.BlockSpec(memory_space=pl.ANY)] * 5,
            out_specs=pl.BlockSpec(memory_space=pltpu.VMEM),
            scratch_shapes=[
                pltpu.VMEM((tokens, width), hidden.dtype),
                pltpu.VMEM((RING, CHUNK, width), embedding.dtype),
                pltpu.VMEM((CHUNK, tokens), F32),
                pltpu.VMEM((1, width), F32),
                pltpu.VMEM((1, width), F32),
                pltpu.VMEM((1, tokens), jnp.int32),
                pltpu.VMEM((tokens, LANES), F32),
                pltpu.VMEM((tokens, LANES), F32),
                pltpu.VMEM((tokens, LANES), F32),
                pltpu.VMEM((2, 8, tokens), F32),
                pltpu.VMEM((8, tokens), F32),
                pltpu.VMEM((8, tokens), F32),
                pltpu.SemaphoreType.DMA((3,)),
                pltpu.SemaphoreType.DMA((HID_PARTS,)),
                pltpu.SemaphoreType.DMA((RING,)),
                pltpu.SemaphoreType.DMA((FIRST, PARTS)),
                pltpu.SemaphoreType.DMA((2, PARTS)),
            ],
            compiler_params=pltpu.CompilerParams(vmem_limit_bytes=HEAD_VMEM),
            name="head",
        )(*[pltpu.with_memory_space_constraint(x, pltpu.HBM) for x in (
            hidden, ln_gain.reshape(1, width), ln_bias.reshape(1, width), embedding, targets)])
        vmem = pl.BlockSpec(memory_space=pltpu.VMEM)
        boxes = pl.pallas_call(
            functools.partial(exchange_kernel, n_tp),
            out_shape=jax.ShapeDtypeStruct((n_tp, 1, 3 * tokens), F32),
            in_specs=[vmem],
            out_specs=vmem,
            scratch_shapes=[
                pltpu.VMEM((n_tp, 1, 3 * tokens), F32),
                pltpu.SemaphoreType.DMA((n_tp,)),
                pltpu.SemaphoreType.DMA((n_tp,)),
            ],
            compiler_params=pltpu.CompilerParams(
                collective_id=0, has_side_effects=True, vmem_limit_bytes=SMALL_VMEM),
            name="exchange",
        )(stats)
        log_norm, token_logp, seq, top_logp = pl.pallas_call(
            finish_kernel,
            out_shape=(row, row, jax.ShapeDtypeStruct((prompts, LANES), F32), row),
            in_specs=[vmem] * 2,
            out_specs=[vmem] * 4,
            compiler_params=pltpu.CompilerParams(vmem_limit_bytes=SMALL_VMEM),
            name="finish",
        )(boxes, score_mask)
        return log_norm, token_logp, seq[:, 0], top_logp

    row_spec = P("dp", None)
    return jax.shard_map(local_part, mesh=mesh,
                         in_specs=(P("dp", None, None), P(), P(), P("tp", None), row_spec, row_spec),
                         out_specs=(row_spec, row_spec, P("dp"), row_spec), check_vma=False)
```

```python
import functools

import jax
import jax.numpy as jnp
from jax import lax
from jax.experimental import pallas as pl
from jax.experimental.pallas import tpu as pltpu
from jax.sharding import PartitionSpec as P

OPT_VOCAB = 50272
LN_EPS = 1e-5

TILE = 256
CHUNK = 256
PIECE = 64
LANES = 128
RING = 8
FIRST = 3
PARTS = 6
HID_PARTS = 4
NORM_ROWS = 32
HEAD_VMEM = 52 << 20
SMALL_VMEM = 1 << 20
F32 = jnp.float32


def head_kernel(hid_hbm, gain_hbm, bias_hbm, emb_hbm, tgt_hbm, stats_ref,
                h, ring, z, gain, bias, tgt, mean_b, rstd_b, part, m8, s8, t8, small_sem, hid_sem, ring_sem,
                first_sem, last_sem):
    tokens, width = h.shape
    rows = emb_hbm.shape[0]
    n_chunks = rows // CHUNK
    passes = width // (2 * TILE)
    part_width = width // PARTS
    part_passes = passes // PARTS
    hid_rows = tokens // HID_PARTS
    base = lax.axis_index("tp") * rows

    def hid_copy(i):
        at = pl.ds(i * hid_rows, hid_rows)
        return pltpu.make_async_copy(hid_hbm.at[0, at], h.at[at], hid_sem.at[i])

    def chunk_copy(c):
        slot = lax.rem(c, RING)
        return pltpu.make_async_copy(emb_hbm.at[pl.ds(c * CHUNK, CHUNK)], ring.at[slot], ring_sem.at[slot])

    def part_copy(c, i, sem):
        cols = pl.ds(i * part_width, part_width)
        return pltpu.make_async_copy(
            emb_hbm.at[pl.ds(c * CHUNK, CHUNK), cols], ring.at[lax.rem(c, RING), :, cols], sem)

    def first_copy(e, i):
        return part_copy(e, i, first_sem.at[e, i])

    def last_copy(e, i):
        return part_copy(n_chunks - 2 + e, i, last_sem.at[e, i])

    small = [pltpu.make_async_copy(src, dst, small_sem.at[i]) for i, (src, dst) in enumerate(
        ((gain_hbm, gain), (bias_hbm, bias), (tgt_hbm, tgt)))]

    for i in range(HID_PARTS):
        hid_copy(i).start()
    for copy in small:
        copy.start()
    early = list(range(FIRST, RING))

    def lane_sum(r, n, fn):
        acc = [jnp.zeros((n, LANES), F32) for _ in range(2)]
        for c in range(width // LANES):
            acc[c % 2] += fn(h[pl.ds(r, n), pl.ds(c * LANES, LANES)].astype(F32))
        return acc[0] + acc[1]

    group = 16

    def mean_rows(i):
        for g in range(hid_rows // group):
            r = i * hid_rows + g * group
            part[pl.ds(r, group)] = lane_sum(r, group, lambda x: x)
        at = pl.ds(i * hid_rows, hid_rows)
        mean = jnp.sum(part[at], axis=-1, keepdims=True) * (1.0 / width)
        mean_b[at] = jnp.broadcast_to(mean, (hid_rows, LANES))

    def var_rows(i):
        for g in range(hid_rows // group):
            r = i * hid_rows + g * group
            mean = mean_b[pl.ds(r, group)]
            part[pl.ds(r, group)] = lane_sum(r, group, lambda x: (x - mean) * (x - mean))
        at = pl.ds(i * hid_rows, hid_rows)
        var = jnp.sum(part[at], axis=-1, keepdims=True) * (1.0 / width)
        rstd_b[at] = jnp.broadcast_to(lax.rsqrt(var + LN_EPS), (hid_rows, LANES))

    for i in range(HID_PARTS):
        hid_copy(i).wait()
        if i == 0:
            for k in range(PARTS):
                for e in range(FIRST):
                    first_copy(e, k).start(priority=1)
        mean_rows(i)
        if i:
            var_rows(i - 1)
    chunk_copy(early.pop(0)).start(priority=1)
    var_rows(HID_PARTS - 1)

    for copy in small:
        copy.wait()
    m8[...] = jnp.full_like(m8, jnp.finfo(F32).min)
    s8[...] = jnp.zeros_like(s8)
    t8[...] = jnp.zeros_like(t8)

    def normalize(k, r=0, n=tokens):
        at, cols = pl.ds(r, n), pl.ds(k * TILE, TILE)
        wide = lambda x: jnp.concatenate([x] * (TILE // LANES), axis=1)
        x = h[at, cols].astype(F32)
        x = (x - wide(mean_b[at])) * wide(rstd_b[at]) * gain[:, cols] + bias[:, cols]
        h[at, cols] = x.astype(h.dtype)

    def matmuls(*accs):
        n_piece = CHUNK // PIECE
        accs = [[accs[(w * 2 + q) * n_piece:(w * 2 + q + 1) * n_piece] for q in range(2)] for w in range(4)]

        for which in accs:
            for q in which:
                for acc in q:
                    z[pl.ds(0, PIECE)] = pltpu.matmul_pop(acc)

        def push(j, q):
            cols = pl.ds((2 * j + q) * TILE, TILE)
            pltpu.matmul_push_rhs(h[:, cols], staging_register=j % 2, mxu_index=q, transpose=True)

        def accumulate(chunks, sets, j):
            def step(c, which, p, q):
                lhs = ring[lax.rem(c, RING), pl.ds(p * PIECE, PIECE), pl.ds((2 * j + q) * TILE, TILE)]
                pltpu.matmul_acc_lhs(
                    accs[which][q][p], lhs, load_staged_rhs=j % 2 if which == sets[0] and p == 0 else None)
            return [functools.partial(step, c, which, p, q)
                    for c, which in zip(chunks, sets) for p in range(n_piece) for q in range(2)]

        def drain(c, which, p):
            offset = base + c * CHUNK
            target = tgt[...] - offset
            limit = OPT_VOCAB - offset
            shape = (PIECE // 8, 8, tokens)
            logits = pltpu.matmul_pop(accs[which][0][p]) + pltpu.matmul_pop(accs[which][1][p])
            row = lax.broadcasted_iota(jnp.int32, logits.shape, 0) + p * PIECE
            logits = jnp.where(row < limit, logits, -jnp.inf)
            z[pl.ds(p * PIECE, PIECE)] = logits
            m8[1] = jnp.maximum(m8[1], jnp.max(logits.reshape(shape), axis=0))
            t8[...] += jnp.sum(jnp.where(row == target, logits, 0.0).reshape(shape), axis=0)

        def exps(p):
            top = m8[1]
            total = s8[...]
            if p == 0:
                total = total * jnp.exp(m8[0] - top)
                m8[0] = top
            e = jnp.exp(z[pl.ds(p * PIECE, PIECE)].reshape(PIECE // 8, 8, tokens) - top[None])
            s8[...] = total + jnp.sum(e, axis=0)

        def absorb(c, which):
            return [functools.partial(drain, c, which, p) for p in range(n_piece)] + [
                functools.partial(exps, p) for p in range(n_piece)]

        def sweep(chunks, sets, beside=(), hooks=None, norm=False, last=False):
            beside = list(beside)
            per_pass = pl.cdiv(len(beside), passes - 3)
            for j in range(passes):
                if hooks and j in hooks:
                    hooks[j]()
                def push_next():
                    for q in range(2):
                        if not (last and j + 1 == passes):
                            push((j + 1) % passes, q)

                steps = accumulate(chunks, sets, j)
                if norm and j + 1 < passes:
                    cut = len(steps) * 2 // 3
                    groups = [(2 * (j + 1) + q, r) for q in range(2) for r in range(0, tokens, NORM_ROWS)]
                    for i, step in enumerate(steps):
                        for k, r in groups[i * len(groups) // cut:(i + 1) * len(groups) // cut]:
                            normalize(k, r, NORM_ROWS)
                        if i == cut:
                            push_next()
                        step()
                else:
                    push_next()
                    for step in steps:
                        step()
                if j >= 2:
                    for step in beside[(j - 2) * per_pass:(j - 1) * per_pass]:
                        step()

        def first_wait(i):
            for e in range(FIRST):
                first_copy(e, i).wait()
            for _ in range(len(early) - (PARTS - 1 - i) * len(early) // (PARTS - i)):
                chunk_copy(early.pop(0)).start(priority=1)

        def last_wait(i):
            for e in range(2):
                last_copy(e, i).wait()

        def part_hooks(wait):
            return {part_passes * i - 1: functools.partial(wait, i) for i in range(1, PARTS)}

        def chunk_wait(c):
            for e in range(2):
                chunk_copy(c + e).wait()

        for k in range(2):
            normalize(k)
        for q in range(2):
            push(0, q)
        first_wait(0)
        sweep(range(FIRST), range(FIRST), norm=True,
              hooks={**part_hooks(first_wait), passes - 1: functools.partial(chunk_wait, FIRST)})
        for step in absorb(0, 0):
            step()
        for c in range(RING, RING + FIRST - 2):
            chunk_copy(c).start(priority=1)

        def pair(c, sets, old, refill=None, ahead=chunk_wait):
            def turn():
                if refill is not None:
                    refill(c - 2 + RING)
                ahead(c + 2)

            sweep((c, c + 1), sets, absorb(c - 2, old[0]) + absorb(c - 1, old[1]), hooks={passes - 2: turn})

        def refill(c):
            for e in range(2):
                chunk_copy(c + e).start(priority=1)

        def refill_or_last(c):
            @pl.when(c < n_chunks - 2)
            def _():
                refill(c)

            @pl.when(c == n_chunks - 2)
            def _():
                for i in range(PARTS):
                    for e in range(2):
                        last_copy(e, i).start(priority=1)

        def two_pairs(i, carry):
            c = FIRST + 4 * i
            pair(c, (3, 0), (1, 2), refill)
            pair(c + 2, (1, 2), (3, 0), refill_or_last)
            return carry

        trips = (n_chunks - FIRST) // 4 - 1
        lax.fori_loop(0, trips, two_pairs, 0)
        c = FIRST + 4 * trips
        pair(c, (3, 0), (1, 2))
        pair(c + 2, (1, 2), (3, 0), ahead=lambda _: last_wait(0))
        c = n_chunks - 2
        sweep((c, c + 1), (3, 0), absorb(c - 2, 1) + absorb(c - 1, 2), hooks=part_hooks(last_wait), last=True)
        for step in absorb(c, 3) + absorb(c + 1, 0):
            step()

    pl.run_scoped(matmuls, *[pltpu.ACC(q)((PIECE, TILE), F32)
                             for _ in range(4) for q in range(2) for _ in range(CHUNK // PIECE)])

    top = jnp.max(m8[0], axis=0, keepdims=True)
    total = jnp.sum(s8[...] * jnp.exp(m8[0] - top), axis=0, keepdims=True)
    picked = jnp.sum(t8[...], axis=0, keepdims=True)
    stats_ref[...] = jnp.concatenate([top, total, picked], axis=1)


def exchange_kernel(n_tp, stats_ref, out_ref, box, send_sem, recv_sem):
    me = lax.axis_index("tp")

    def peer(d):
        return lax.rem(me + d, n_tp)

    def exchange(d, slot):
        return pltpu.make_async_remote_copy(
            src_ref=stats_ref, dst_ref=box.at[slot], send_sem=send_sem.at[d], recv_sem=recv_sem.at[slot],
            device_id={"tp": peer(d)}, device_id_type=pl.DeviceIdType.MESH)

    barrier = pltpu.get_barrier_semaphore()
    for d in range(1, n_tp):
        pl.semaphore_signal(barrier, inc=1, device_id={"tp": peer(d)}, device_id_type=pl.DeviceIdType.MESH)
    pl.semaphore_wait(barrier, n_tp - 1)
    for d in range(1, n_tp):
        exchange(d, me).start()
    box[me] = stats_ref[...]
    for d in range(1, n_tp):
        exchange(d, peer(d)).wait_recv()
    out_ref[...] = box[...]
    for d in range(1, n_tp):
        exchange(d, me).wait_send()


def finish_kernel(box, mask, norm_ref, logp_ref, seq_ref, top_ref):
    n_tp, _, width = box.shape
    tokens = width // 3
    boxes = [box[i] for i in range(n_tp)]
    top = functools.reduce(jnp.maximum, [x[:, :tokens] for x in boxes])
    total = sum(x[:, tokens:2 * tokens] * jnp.exp(x[:, :tokens] - top) for x in boxes)
    picked = sum(x[:, 2 * tokens:] for x in boxes)
    log_norm = top + jnp.log(total)
    token_logp = (picked - log_norm) * mask[...].astype(F32)
    norm_ref[...] = log_norm
    logp_ref[...] = token_logp
    top_ref[...] = top - log_norm
    seq_ref[...] = jnp.broadcast_to(jnp.sum(token_logp, axis=-1, keepdims=True), seq_ref.shape)


def solution(mesh):
    n_tp = mesh.shape["tp"]

    def local_part(hidden, ln_gain, ln_bias, embedding, targets, score_mask):
        prompts, tokens, width = hidden.shape
        rows = embedding.shape[0]
        n_chunks = rows // CHUNK
        assert prompts == 1 and tokens == TILE and rows % CHUNK == 0 and width % (2 * TILE * PARTS) == 0
        assert (n_chunks - FIRST) % 4 == 2 and n_chunks == RING + FIRST + 4 * ((n_chunks - FIRST) // 4 - 1) - 2
        row = jax.ShapeDtypeStruct((prompts, tokens), F32)
        stats = pl.pallas_call(
            head_kernel,
            out_shape=jax.ShapeDtypeStruct((1, 3 * tokens), F32),
            in_specs=[pl.BlockSpec(memory_space=pl.ANY)] * 5,
            out_specs=pl.BlockSpec(memory_space=pltpu.VMEM),
            scratch_shapes=[
                pltpu.VMEM((tokens, width), hidden.dtype),
                pltpu.VMEM((RING, CHUNK, width), embedding.dtype),
                pltpu.VMEM((CHUNK, tokens), F32),
                pltpu.VMEM((1, width), F32),
                pltpu.VMEM((1, width), F32),
                pltpu.VMEM((1, tokens), jnp.int32),
                pltpu.VMEM((tokens, LANES), F32),
                pltpu.VMEM((tokens, LANES), F32),
                pltpu.VMEM((tokens, LANES), F32),
                pltpu.VMEM((2, 8, tokens), F32),
                pltpu.VMEM((8, tokens), F32),
                pltpu.VMEM((8, tokens), F32),
                pltpu.SemaphoreType.DMA((3,)),
                pltpu.SemaphoreType.DMA((HID_PARTS,)),
                pltpu.SemaphoreType.DMA((RING,)),
                pltpu.SemaphoreType.DMA((FIRST, PARTS)),
                pltpu.SemaphoreType.DMA((2, PARTS)),
            ],
            compiler_params=pltpu.CompilerParams(vmem_limit_bytes=HEAD_VMEM),
            name="head",
        )(*[pltpu.with_memory_space_constraint(x, pltpu.HBM) for x in (
            hidden, ln_gain.reshape(1, width), ln_bias.reshape(1, width), embedding, targets)])
        vmem = pl.BlockSpec(memory_space=pltpu.VMEM)
        boxes = pl.pallas_call(
            functools.partial(exchange_kernel, n_tp),
            out_shape=jax.ShapeDtypeStruct((n_tp, 1, 3 * tokens), F32),
            in_specs=[vmem],
            out_specs=vmem,
            scratch_shapes=[
                pltpu.VMEM((n_tp, 1, 3 * tokens), F32),
                pltpu.SemaphoreType.DMA((n_tp,)),
                pltpu.SemaphoreType.DMA((n_tp,)),
            ],
            compiler_params=pltpu.CompilerParams(
                collective_id=0, has_side_effects=True, vmem_limit_bytes=SMALL_VMEM),
            name="exchange",
        )(stats)
        log_norm, token_logp, seq, top_logp = pl.pallas_call(
            finish_kernel,
            out_shape=(row, row, jax.ShapeDtypeStruct((prompts, LANES), F32), row),
            in_specs=[vmem] * 2,
            out_specs=[vmem] * 4,
            compiler_params=pltpu.CompilerParams(vmem_limit_bytes=SMALL_VMEM),
            name="finish",
        )(boxes, score_mask)
        return log_norm, token_logp, seq[:, 0], top_logp

    row_spec = P("dp", None)
    return jax.shard_map(local_part, mesh=mesh,
                         in_specs=(P("dp", None, None), P(), P(), P("tp", None), row_spec, row_spec),
                         out_specs=(row_spec, row_spec, P("dp"), row_spec), check_vma=False)
```

```python
import functools

import jax
import jax.numpy as jnp
from jax import lax
from jax.experimental import pallas as pl
from jax.experimental.pallas import tpu as pltpu
from jax.sharding import PartitionSpec as P

OPT_VOCAB = 50272
LN_EPS = 1e-5

TILE = 256
CHUNK = 256
PIECE = 64
LANES = 128
RING = 8
FIRST = 3
PARTS = 6
HID_PARTS = 4
NORM_ROWS = 32
HEAD_VMEM = 52 << 20
SMALL_VMEM = 1 << 20
F32 = jnp.float32


def head_kernel(hid_hbm, gain_hbm, bias_hbm, emb_hbm, tgt_hbm, stats_ref,
                h, ring, z, gain, bias, tgt, mean_b, rstd_b, part, m8, s8, t8, small_sem, hid_sem, ring_sem,
                first_sem, last_sem):
    tokens, width = h.shape
    rows = emb_hbm.shape[0]
    n_chunks = rows // CHUNK
    passes = width // (2 * TILE)
    part_width = width // PARTS
    part_passes = passes // PARTS
    hid_rows = tokens // HID_PARTS
    base = lax.axis_index("tp") * rows

    def hid_copy(i):
        at = pl.ds(i * hid_rows, hid_rows)
        return pltpu.make_async_copy(hid_hbm.at[0, at], h.at[at], hid_sem.at[i])

    def slot(c):
        return lax.rem(c + 1, RING)

    def pair_copy(c):
        at = pl.ds(pl.multiple_of(c * CHUNK, CHUNK), 2 * CHUNK)
        to = pl.ds(pl.multiple_of(slot(c) * CHUNK, CHUNK), 2 * CHUNK)
        return pltpu.make_async_copy(emb_hbm.at[at], ring.at[to], ring_sem.at[slot(c)])

    def part_copy(c, i, sem):
        at = pl.ds(pl.multiple_of(c * CHUNK, CHUNK), CHUNK)
        to = pl.ds(pl.multiple_of(slot(c) * CHUNK, CHUNK), CHUNK)
        cols = pl.ds(i * part_width, part_width)
        return pltpu.make_async_copy(emb_hbm.at[at, cols], ring.at[to, cols], sem)

    def first_copy(e, i):
        return part_copy(e, i, first_sem.at[e, i])

    def last_copy(e, i):
        return part_copy(n_chunks - 2 + e, i, last_sem.at[e, i])

    small = [pltpu.make_async_copy(src, dst, small_sem.at[i]) for i, (src, dst) in enumerate(
        ((gain_hbm, gain), (bias_hbm, bias), (tgt_hbm, tgt)))]

    for i in range(HID_PARTS):
        hid_copy(i).start()
    for copy in small:
        copy.start()
    early = list(range(FIRST, RING - 2, 2))

    def lane_sum(r, n, fn):
        acc = [jnp.zeros((n, LANES), F32) for _ in range(2)]
        for c in range(width // LANES):
            acc[c % 2] += fn(h[pl.ds(r, n), pl.ds(c * LANES, LANES)].astype(F32))
        return acc[0] + acc[1]

    group = 16

    def mean_rows(i):
        for g in range(hid_rows // group):
            r = i * hid_rows + g * group
            part[pl.ds(r, group)] = lane_sum(r, group, lambda x: x)
        at = pl.ds(i * hid_rows, hid_rows)
        mean = jnp.sum(part[at], axis=-1, keepdims=True) * (1.0 / width)
        mean_b[at] = jnp.broadcast_to(mean, (hid_rows, LANES))

    def var_rows(i):
        for g in range(hid_rows // group):
            r = i * hid_rows + g * group
            mean = mean_b[pl.ds(r, group)]
            part[pl.ds(r, group)] = lane_sum(r, group, lambda x: (x - mean) * (x - mean))
        at = pl.ds(i * hid_rows, hid_rows)
        var = jnp.sum(part[at], axis=-1, keepdims=True) * (1.0 / width)
        rstd_b[at] = jnp.broadcast_to(lax.rsqrt(var + LN_EPS), (hid_rows, LANES))

    for i in range(HID_PARTS):
        hid_copy(i).wait()
        if i == 0:
            for k in range(PARTS):
                for e in range(FIRST):
                    first_copy(e, k).start(priority=1)
        mean_rows(i)
        if i:
            var_rows(i - 1)
    pair_copy(early.pop(0)).start(priority=1)
    var_rows(HID_PARTS - 1)

    for copy in small:
        copy.wait()
    m8[...] = jnp.full_like(m8, jnp.finfo(F32).min)
    s8[...] = jnp.zeros_like(s8)
    t8[...] = jnp.zeros_like(t8)

    def normalize(k, r=0, n=tokens):
        at, cols = pl.ds(r, n), pl.ds(k * TILE, TILE)
        wide = lambda x: jnp.concatenate([x] * (TILE // LANES), axis=1)
        x = h[at, cols].astype(F32)
        x = (x - wide(mean_b[at])) * wide(rstd_b[at]) * gain[:, cols] + bias[:, cols]
        h[at, cols] = x.astype(h.dtype)

    def matmuls(*accs):
        n_piece = CHUNK // PIECE
        accs = [[accs[(w * 2 + q) * n_piece:(w * 2 + q + 1) * n_piece] for q in range(2)] for w in range(4)]

        for which in accs:
            for q in which:
                for acc in q:
                    z[pl.ds(0, PIECE)] = pltpu.matmul_pop(acc)

        def push(j, q):
            cols = pl.ds((2 * j + q) * TILE, TILE)
            pltpu.matmul_push_rhs(h[:, cols], staging_register=j % 2, mxu_index=q, transpose=True)

        def accumulate(chunks, sets, j):
            def step(c, which, p, q):
                at = pl.ds(pl.multiple_of(slot(c) * CHUNK + p * PIECE, PIECE), PIECE)
                lhs = ring[at, pl.ds((2 * j + q) * TILE, TILE)]
                pltpu.matmul_acc_lhs(
                    accs[which][q][p], lhs, load_staged_rhs=j % 2 if which == sets[0] and p == 0 else None)
            return [functools.partial(step, c, which, p, q)
                    for c, which in zip(chunks, sets) for p in range(n_piece) for q in range(2)]

        def drain(c, which, p):
            offset = base + c * CHUNK
            target = tgt[...] - offset
            limit = OPT_VOCAB - offset
            shape = (PIECE // 8, 8, tokens)
            logits = pltpu.matmul_pop(accs[which][0][p]) + pltpu.matmul_pop(accs[which][1][p])
            row = lax.broadcasted_iota(jnp.int32, logits.shape, 0) + p * PIECE
            logits = jnp.where(row < limit, logits, -jnp.inf)
            z[pl.ds(p * PIECE, PIECE)] = logits
            m8[1] = jnp.maximum(m8[1], jnp.max(logits.reshape(shape), axis=0))
            t8[...] += jnp.sum(jnp.where(row == target, logits, 0.0).reshape(shape), axis=0)

        def exps(p):
            top = m8[1]
            total = s8[...]
            if p == 0:
                total = total * jnp.exp(m8[0] - top)
                m8[0] = top
            e = jnp.exp(z[pl.ds(p * PIECE, PIECE)].reshape(PIECE // 8, 8, tokens) - top[None])
            s8[...] = total + jnp.sum(e, axis=0)

        def absorb(c, which):
            return [functools.partial(drain, c, which, p) for p in range(n_piece)] + [
                functools.partial(exps, p) for p in range(n_piece)]

        def sweep(chunks, sets, beside=(), wait=None, norm=False, last=False):
            beside = list(beside)
            per_pass = pl.cdiv(len(beside), passes - 3)
            for j in range(passes):
                if wait is not None and j % part_passes == 0:
                    wait(j // part_passes)
                def push_next():
                    for q in range(2):
                        if not (last and j + 1 == passes):
                            push((j + 1) % passes, q)

                steps = accumulate(chunks, sets, j)
                if norm and j + 1 < passes:
                    cut = len(steps) * 2 // 3
                    groups = [(2 * (j + 1) + q, r) for q in range(2) for r in range(0, tokens, NORM_ROWS)]
                    for i, step in enumerate(steps):
                        for k, r in groups[i * len(groups) // cut:(i + 1) * len(groups) // cut]:
                            normalize(k, r, NORM_ROWS)
                        if i == cut:
                            push_next()
                        step()
                else:
                    push_next()
                    for step in steps:
                        step()
                if j >= 2:
                    for step in beside[(j - 2) * per_pass:(j - 1) * per_pass]:
                        step()

        def first_wait(i):
            for e in range(FIRST):
                first_copy(e, i).wait()
            if i % 3 == 1 and early:
                pair_copy(early.pop(0)).start(priority=1)

        for k in range(2):
            normalize(k)
        for q in range(2):
            push(0, q)
        sweep(range(FIRST), range(FIRST), wait=first_wait, norm=True)
        for step in absorb(0, 0):
            step()
        pair_copy(FIRST - 4 + RING).start(priority=1)
        def refill(c):
            @pl.when(c < n_chunks - 2)
            def _():
                pair_copy(c).start(priority=1)

            @pl.when(c == n_chunks - 2)
            def _():
                for e in range(2):
                    for i in range(PARTS):
                        last_copy(e, i).start(priority=1)

        def pair(c, sets, old):
            pair_copy(c).wait()
            refill(c - 2 + RING)
            sweep((c, c + 1), sets, absorb(c - 2, old[0]) + absorb(c - 1, old[1]))

        def two_pairs(i, carry):
            c = FIRST + 4 * i
            pair(c, (3, 0), (1, 2))
            pair(c + 2, (1, 2), (3, 0))
            return carry

        lax.fori_loop(0, (n_chunks - FIRST - 2) // 4, two_pairs, 0)
        c = n_chunks - 2
        sweep((c,), (3,), absorb(c - 2, 1) + absorb(c - 1, 2), wait=lambda i: last_copy(0, i).wait())
        sweep((c + 1,), (0,), absorb(c, 3), wait=lambda i: last_copy(1, i).wait(), last=True)
        for step in absorb(c + 1, 0):
            step()

    pl.run_scoped(matmuls, *[pltpu.ACC(q)((PIECE, TILE), F32)
                             for _ in range(4) for q in range(2) for _ in range(CHUNK // PIECE)])

    top = jnp.max(m8[0], axis=0, keepdims=True)
    total = jnp.sum(s8[...] * jnp.exp(m8[0] - top), axis=0, keepdims=True)
    picked = jnp.sum(t8[...], axis=0, keepdims=True)
    stats_ref[...] = jnp.concatenate([top, total, picked], axis=1)


def exchange_kernel(n_tp, stats_ref, out_ref, box, send_sem, recv_sem):
    me = lax.axis_index("tp")

    def peer(d):
        return lax.rem(me + d, n_tp)

    def exchange(d, slot):
        return pltpu.make_async_remote_copy(
            src_ref=stats_ref, dst_ref=box.at[slot], send_sem=send_sem.at[d], recv_sem=recv_sem.at[slot],
            device_id={"tp": peer(d)}, device_id_type=pl.DeviceIdType.MESH)

    barrier = pltpu.get_barrier_semaphore()
    for d in range(1, n_tp):
        pl.semaphore_signal(barrier, inc=1, device_id={"tp": peer(d)}, device_id_type=pl.DeviceIdType.MESH)
    pl.semaphore_wait(barrier, n_tp - 1)
    for d in range(1, n_tp):
        exchange(d, me).start()
    box[me] = stats_ref[...]
    for d in range(1, n_tp):
        exchange(d, peer(d)).wait_recv()
    out_ref[...] = box[...]
    for d in range(1, n_tp):
        exchange(d, me).wait_send()


def finish_kernel(box, mask, norm_ref, logp_ref, seq_ref, top_ref):
    n_tp, _, width = box.shape
    tokens = width // 3
    boxes = [box[i] for i in range(n_tp)]
    top = functools.reduce(jnp.maximum, [x[:, :tokens] for x in boxes])
    total = sum(x[:, tokens:2 * tokens] * jnp.exp(x[:, :tokens] - top) for x in boxes)
    picked = sum(x[:, 2 * tokens:] for x in boxes)
    log_norm = top + jnp.log(total)
    token_logp = (picked - log_norm) * mask[...].astype(F32)
    norm_ref[...] = log_norm
    logp_ref[...] = token_logp
    top_ref[...] = top - log_norm
    seq_ref[...] = jnp.broadcast_to(jnp.sum(token_logp, axis=-1, keepdims=True), seq_ref.shape)


def solution(mesh):
    n_tp = mesh.shape["tp"]

    def local_part(hidden, ln_gain, ln_bias, embedding, targets, score_mask):
        prompts, tokens, width = hidden.shape
        rows = embedding.shape[0]
        n_chunks = rows // CHUNK
        assert prompts == 1 and tokens == TILE and rows % CHUNK == 0 and width % (2 * TILE * PARTS) == 0
        assert (n_chunks - FIRST) % 4 == 2 and n_chunks > RING + FIRST and RING % 2 == 0
        row = jax.ShapeDtypeStruct((prompts, tokens), F32)
        stats = pl.pallas_call(
            head_kernel,
            out_shape=jax.ShapeDtypeStruct((1, 3 * tokens), F32),
            in_specs=[pl.BlockSpec(memory_space=pl.ANY)] * 5,
            out_specs=pl.BlockSpec(memory_space=pltpu.VMEM),
            scratch_shapes=[
                pltpu.VMEM((tokens, width), hidden.dtype),
                pltpu.VMEM((RING * CHUNK, width), embedding.dtype),
                pltpu.VMEM((CHUNK, tokens), F32),
                pltpu.VMEM((1, width), F32),
                pltpu.VMEM((1, width), F32),
                pltpu.VMEM((1, tokens), jnp.int32),
                pltpu.VMEM((tokens, LANES), F32),
                pltpu.VMEM((tokens, LANES), F32),
                pltpu.VMEM((tokens, LANES), F32),
                pltpu.VMEM((2, 8, tokens), F32),
                pltpu.VMEM((8, tokens), F32),
                pltpu.VMEM((8, tokens), F32),
                pltpu.SemaphoreType.DMA((3,)),
                pltpu.SemaphoreType.DMA((HID_PARTS,)),
                pltpu.SemaphoreType.DMA((RING,)),
                pltpu.SemaphoreType.DMA((FIRST, PARTS)),
                pltpu.SemaphoreType.DMA((2, PARTS)),
            ],
            compiler_params=pltpu.CompilerParams(vmem_limit_bytes=HEAD_VMEM),
            name="head",
        )(*[pltpu.with_memory_space_constraint(x, pltpu.HBM) for x in (
            hidden, ln_gain.reshape(1, width), ln_bias.reshape(1, width), embedding, targets)])
        vmem = pl.BlockSpec(memory_space=pltpu.VMEM)
        boxes = pl.pallas_call(
            functools.partial(exchange_kernel, n_tp),
            out_shape=jax.ShapeDtypeStruct((n_tp, 1, 3 * tokens), F32),
            in_specs=[vmem],
            out_specs=vmem,
            scratch_shapes=[
                pltpu.VMEM((n_tp, 1, 3 * tokens), F32),
                pltpu.SemaphoreType.DMA((n_tp,)),
                pltpu.SemaphoreType.DMA((n_tp,)),
            ],
            compiler_params=pltpu.CompilerParams(
                collective_id=0, has_side_effects=True, vmem_limit_bytes=SMALL_VMEM),
            name="exchange",
        )(stats)
        log_norm, token_logp, seq, top_logp = pl.pallas_call(
            finish_kernel,
            out_shape=(row, row, jax.ShapeDtypeStruct((prompts, LANES), F32), row),
            in_specs=[vmem] * 2,
            out_specs=[vmem] * 4,
            compiler_params=pltpu.CompilerParams(vmem_limit_bytes=SMALL_VMEM),
            name="finish",
        )(boxes, score_mask)
        return log_norm, token_logp, seq[:, 0], top_logp

    row_spec = P("dp", None)
    return jax.shard_map(local_part, mesh=mesh,
                         in_specs=(P("dp", None, None), P(), P(), P("tp", None), row_spec, row_spec),
                         out_specs=(row_spec, row_spec, P("dp"), row_spec), check_vma=False)
```

```python
import functools

import jax
import jax.numpy as jnp
from jax import lax
from jax.experimental import pallas as pl
from jax.experimental.pallas import tpu as pltpu
from jax.sharding import PartitionSpec as P

OPT_VOCAB = 50272
LN_EPS = 1e-5

TILE = 256
CHUNK = 256
PIECE = 32
LANES = 128
RING = 8
FIRST = 3
PARTS = 6
HID_PARTS = 8
NORM_ROWS = 32
HEAD_VMEM = 52 << 20
SMALL_VMEM = 1 << 20
F32 = jnp.float32


def head_kernel(hid_hbm, gain_hbm, bias_hbm, emb_hbm, tgt_hbm, stats_ref,
                h, ring, z, gain, bias, tgt, mean_b, rstd_b, part, m8, s8, t8, small_sem, hid_sem, ring_sem,
                first_sem, last_sem):
    tokens, width = h.shape
    rows = emb_hbm.shape[0]
    n_chunks = rows // CHUNK
    passes = width // (2 * TILE)
    part_width = width // PARTS
    part_passes = passes // PARTS
    hid_rows = tokens // HID_PARTS
    base = lax.axis_index("tp") * rows

    def hid_copy(i):
        at = pl.ds(i * hid_rows, hid_rows)
        return pltpu.make_async_copy(hid_hbm.at[0, at], h.at[at], hid_sem.at[i])

    def chunk_copy(c):
        slot = lax.rem(c, RING)
        return pltpu.make_async_copy(emb_hbm.at[pl.ds(c * CHUNK, CHUNK)], ring.at[slot], ring_sem.at[slot])

    def part_copy(c, i, sem):
        cols = pl.ds(i * part_width, part_width)
        return pltpu.make_async_copy(
            emb_hbm.at[pl.ds(c * CHUNK, CHUNK), cols], ring.at[lax.rem(c, RING), :, cols], sem)

    def first_copy(e, i):
        return part_copy(e, i, first_sem.at[e, i])

    def last_copy(e, i):
        return part_copy(n_chunks - 2 + e, i, last_sem.at[e, i])

    small = [pltpu.make_async_copy(src, dst, small_sem.at[i]) for i, (src, dst) in enumerate(
        ((gain_hbm, gain), (bias_hbm, bias), (tgt_hbm, tgt)))]

    for i in range(HID_PARTS):
        hid_copy(i).start()
    for copy in small:
        copy.start()
    early = list(range(FIRST, RING))

    def lane_sum(r, n, fn):
        acc = [jnp.zeros((n, LANES), F32) for _ in range(2)]
        for c in range(width // LANES):
            acc[c % 2] += fn(h[pl.ds(r, n), pl.ds(c * LANES, LANES)].astype(F32))
        return acc[0] + acc[1]

    group = 16

    def groups(i):
        return [i * hid_rows + g * group for g in range(hid_rows // group)]

    def mean_rows(i):
        for r in groups(i):
            part[pl.ds(r, group)] = lane_sum(r, group, lambda x: x)
        at = pl.ds(i * hid_rows, hid_rows)
        mean = jnp.sum(part[at], axis=-1, keepdims=True) * (1.0 / width)
        mean_b[at] = jnp.broadcast_to(mean, (hid_rows, LANES))

    def var_sums(i):
        for r in groups(i):
            mean = mean_b[pl.ds(r, group)]
            rstd_b[pl.ds(r, group)] = lane_sum(r, group, lambda x: (x - mean) * (x - mean))

    def var_rows(i):
        at = pl.ds(i * hid_rows, hid_rows)
        var = jnp.sum(rstd_b[at], axis=-1, keepdims=True) * (1.0 / width)
        rstd_b[at] = jnp.broadcast_to(lax.rsqrt(var + LN_EPS), (hid_rows, LANES))

    for i in range(HID_PARTS):
        hid_copy(i).wait()
        if i == 0:
            for k in range(PARTS):
                for e in range(FIRST):
                    first_copy(e, k).start(priority=1)
        if i > 1:
            var_rows(i - 2)
        mean_rows(i)
        if i:
            var_sums(i - 1)
    chunk_copy(early.pop(0)).start(priority=1)
    var_rows(HID_PARTS - 2)
    var_sums(HID_PARTS - 1)
    var_rows(HID_PARTS - 1)

    for copy in small:
        copy.wait()
    m8[...] = jnp.full_like(m8, jnp.finfo(F32).min)
    s8[...] = jnp.zeros_like(s8)
    t8[...] = jnp.zeros_like(t8)

    def normalize(k, r=0, n=tokens):
        at, cols = pl.ds(r, n), pl.ds(k * TILE, TILE)
        wide = lambda x: jnp.concatenate([x] * (TILE // LANES), axis=1)
        x = h[at, cols].astype(F32)
        x = (x - wide(mean_b[at])) * wide(rstd_b[at]) * gain[:, cols] + bias[:, cols]
        h[at, cols] = x.astype(h.dtype)

    def matmuls(*accs):
        n_piece = CHUNK // PIECE
        accs = [[accs[(w * 2 + q) * n_piece:(w * 2 + q + 1) * n_piece] for q in range(2)] for w in range(4)]

        for which in accs:
            for q in which:
                for acc in q:
                    z[pl.ds(0, PIECE)] = pltpu.matmul_pop(acc)

        def push(j, q):
            cols = pl.ds((2 * j + q) * TILE, TILE)
            pltpu.matmul_push_rhs(h[:, cols], staging_register=j % 2, mxu_index=q, transpose=True)

        def accumulate(chunks, sets, j):
            def step(c, which, p, q):
                lhs = ring[lax.rem(c, RING), pl.ds(p * PIECE, PIECE), pl.ds((2 * j + q) * TILE, TILE)]
                pltpu.matmul_acc_lhs(
                    accs[which][q][p], lhs, load_staged_rhs=j % 2 if which == sets[0] and p == 0 else None)
            return [functools.partial(step, c, which, p, q)
                    for c, which in zip(chunks, sets) for p in range(n_piece) for q in range(2)]

        def drain(c, which, p):
            offset = base + c * CHUNK
            target = tgt[...] - offset
            limit = OPT_VOCAB - offset
            shape = (PIECE // 8, 8, tokens)
            logits = pltpu.matmul_pop(accs[which][0][p]) + pltpu.matmul_pop(accs[which][1][p])
            row = lax.broadcasted_iota(jnp.int32, logits.shape, 0) + p * PIECE
            logits = jnp.where(row < limit, logits, -jnp.inf)
            z[pl.ds(p * PIECE, PIECE)] = logits
            m8[1] = jnp.maximum(m8[1], jnp.max(logits.reshape(shape), axis=0))
            t8[...] += jnp.sum(jnp.where(row == target, logits, 0.0).reshape(shape), axis=0)

        def exps(p):
            top = m8[1]
            total = s8[...]
            if p == 0:
                total = total * jnp.exp(m8[0] - top)
                m8[0] = top
            e = jnp.exp(z[pl.ds(p * PIECE, PIECE)].reshape(PIECE // 8, 8, tokens) - top[None])
            s8[...] = total + jnp.sum(e, axis=0)

        def absorb(c, which):
            return [functools.partial(drain, c, which, p) for p in range(n_piece)] + [
                functools.partial(exps, p) for p in range(n_piece)]

        def sweep(chunks, sets, beside=(), wait=None, norm=False, last=False):
            beside = list(beside)
            per_pass = pl.cdiv(len(beside), passes - 3)
            for j in range(passes):
                if wait is not None and j % part_passes == 0:
                    wait(j // part_passes)
                def push_next():
                    for q in range(2):
                        if not (last and j + 1 == passes):
                            push((j + 1) % passes, q)

                steps = accumulate(chunks, sets, j)
                if norm and j + 1 < passes:
                    cut = len(steps) * 2 // 3
                    groups = [(2 * (j + 1) + q, r) for q in range(2) for r in range(0, tokens, NORM_ROWS)]
                    for i, step in enumerate(steps):
                        for k, r in groups[i * len(groups) // cut:(i + 1) * len(groups) // cut]:
                            normalize(k, r, NORM_ROWS)
                        if i == cut:
                            push_next()
                        step()
                else:
                    push_next()
                    for step in steps:
                        step()
                if j >= 2:
                    for step in beside[(j - 2) * per_pass:(j - 1) * per_pass]:
                        step()

        def first_wait(i):
            for e in range(FIRST):
                first_copy(e, i).wait()
            for _ in range(len(early) - (PARTS - 1 - i) * len(early) // (PARTS - i)):
                chunk_copy(early.pop(0)).start(priority=1)

        def last_wait(i):
            for e in range(2):
                last_copy(e, i).wait()

        for k in range(2):
            normalize(k)
        for q in range(2):
            push(0, q)
        sweep(range(FIRST), range(FIRST), wait=first_wait, norm=True)
        for step in absorb(0, 0):
            step()
        for c in range(RING, RING + FIRST - 2):
            chunk_copy(c).start(priority=1)

        def pair(c, sets, old, refill=True):
            for e in range(2):
                chunk_copy(c + e).wait()
            if refill:
                @pl.when(c + RING < n_chunks)
                def _():
                    for e in range(2):
                        chunk_copy(c - 2 + e + RING).start(priority=1)

                @pl.when(c + RING == n_chunks)
                def _():
                    for i in range(PARTS):
                        for e in range(2):
                            last_copy(e, i).start(priority=1)
            sweep((c, c + 1), sets, absorb(c - 2, old[0]) + absorb(c - 1, old[1]))

        def two_pairs(i, carry):
            c = FIRST + 4 * i
            pair(c, (3, 0), (1, 2))
            pair(c + 2, (1, 2), (3, 0))
            return carry

        lax.fori_loop(0, (n_chunks - FIRST) // 4, two_pairs, 0)
        c = n_chunks - 2
        sweep((c, c + 1), (3, 0), absorb(c - 2, 1) + absorb(c - 1, 2), wait=last_wait, last=True)
        for step in absorb(c, 3) + absorb(c + 1, 0):
            step()

    pl.run_scoped(matmuls, *[pltpu.ACC(q)((PIECE, TILE), F32)
                             for _ in range(4) for q in range(2) for _ in range(CHUNK // PIECE)])

    top = jnp.max(m8[0], axis=0, keepdims=True)
    total = jnp.sum(s8[...] * jnp.exp(m8[0] - top), axis=0, keepdims=True)
    picked = jnp.sum(t8[...], axis=0, keepdims=True)
    stats_ref[...] = jnp.concatenate([top, total, picked], axis=1)


def exchange_kernel(n_tp, stats_ref, out_ref, box, send_sem, recv_sem):
    me = lax.axis_index("tp")

    def peer(d):
        return lax.rem(me + d, n_tp)

    def exchange(d, slot):
        return pltpu.make_async_remote_copy(
            src_ref=stats_ref, dst_ref=box.at[slot], send_sem=send_sem.at[d], recv_sem=recv_sem.at[slot],
            device_id={"tp": peer(d)}, device_id_type=pl.DeviceIdType.MESH)

    barrier = pltpu.get_barrier_semaphore()
    for d in range(1, n_tp):
        pl.semaphore_signal(barrier, inc=1, device_id={"tp": peer(d)}, device_id_type=pl.DeviceIdType.MESH)
    pl.semaphore_wait(barrier, n_tp - 1)
    for d in range(1, n_tp):
        exchange(d, me).start()
    box[me] = stats_ref[...]
    for d in range(1, n_tp):
        exchange(d, peer(d)).wait_recv()
    out_ref[...] = box[...]
    for d in range(1, n_tp):
        exchange(d, me).wait_send()


def finish_kernel(box, mask, norm_ref, logp_ref, seq_ref, top_ref):
    n_tp, _, width = box.shape
    tokens = width // 3
    boxes = [box[i] for i in range(n_tp)]
    top = functools.reduce(jnp.maximum, [x[:, :tokens] for x in boxes])
    total = sum(x[:, tokens:2 * tokens] * jnp.exp(x[:, :tokens] - top) for x in boxes)
    picked = sum(x[:, 2 * tokens:] for x in boxes)
    log_norm = top + jnp.log(total)
    token_logp = (picked - log_norm) * mask[...].astype(F32)
    norm_ref[...] = log_norm
    logp_ref[...] = token_logp
    top_ref[...] = top - log_norm
    seq_ref[...] = jnp.broadcast_to(jnp.sum(token_logp, axis=-1, keepdims=True), seq_ref.shape)


def solution(mesh):
    n_tp = mesh.shape["tp"]

    def local_part(hidden, ln_gain, ln_bias, embedding, targets, score_mask):
        prompts, tokens, width = hidden.shape
        rows = embedding.shape[0]
        n_chunks = rows // CHUNK
        assert prompts == 1 and tokens == TILE and rows % CHUNK == 0 and width % (2 * TILE * PARTS) == 0
        assert (n_chunks - FIRST) % 4 == 2 and n_chunks > RING + FIRST + 2
        row = jax.ShapeDtypeStruct((prompts, tokens), F32)
        stats = pl.pallas_call(
            head_kernel,
            out_shape=jax.ShapeDtypeStruct((1, 3 * tokens), F32),
            in_specs=[pl.BlockSpec(memory_space=pl.ANY)] * 5,
            out_specs=pl.BlockSpec(memory_space=pltpu.VMEM),
            scratch_shapes=[
                pltpu.VMEM((tokens, width), hidden.dtype),
                pltpu.VMEM((RING, CHUNK, width), embedding.dtype),
                pltpu.VMEM((CHUNK, tokens), F32),
                pltpu.VMEM((1, width), F32),
                pltpu.VMEM((1, width), F32),
                pltpu.VMEM((1, tokens), jnp.int32),
                pltpu.VMEM((tokens, LANES), F32),
                pltpu.VMEM((tokens, LANES), F32),
                pltpu.VMEM((tokens, LANES), F32),
                pltpu.VMEM((2, 8, tokens), F32),
                pltpu.VMEM((8, tokens), F32),
                pltpu.VMEM((8, tokens), F32),
                pltpu.SemaphoreType.DMA((3,)),
                pltpu.SemaphoreType.DMA((HID_PARTS,)),
                pltpu.SemaphoreType.DMA((RING,)),
                pltpu.SemaphoreType.DMA((FIRST, PARTS)),
                pltpu.SemaphoreType.DMA((2, PARTS)),
            ],
            compiler_params=pltpu.CompilerParams(
                vmem_limit_bytes=HEAD_VMEM),
            name="head",
        )(*[pltpu.with_memory_space_constraint(x, pltpu.HBM) for x in (
            hidden, ln_gain.reshape(1, width), ln_bias.reshape(1, width), embedding, targets)])
        vmem = pl.BlockSpec(memory_space=pltpu.VMEM)
        boxes = pl.pallas_call(
            functools.partial(exchange_kernel, n_tp),
            out_shape=jax.ShapeDtypeStruct((n_tp, 1, 3 * tokens), F32),
            in_specs=[vmem],
            out_specs=vmem,
            scratch_shapes=[
                pltpu.VMEM((n_tp, 1, 3 * tokens), F32),
                pltpu.SemaphoreType.DMA((n_tp,)),
                pltpu.SemaphoreType.DMA((n_tp,)),
            ],
            compiler_params=pltpu.CompilerParams(
                collective_id=0, has_side_effects=True, vmem_limit_bytes=SMALL_VMEM),
            name="exchange",
        )(stats)
        log_norm, token_logp, seq, top_logp = pl.pallas_call(
            finish_kernel,
            out_shape=(row, row, jax.ShapeDtypeStruct((prompts, LANES), F32), row),
            in_specs=[vmem] * 2,
            out_specs=[vmem] * 4,
            compiler_params=pltpu.CompilerParams(vmem_limit_bytes=SMALL_VMEM),
            name="finish",
        )(boxes, score_mask)
        return log_norm, token_logp, seq[:, 0], top_logp

    row_spec = P("dp", None)
    return jax.shard_map(local_part, mesh=mesh,
                         in_specs=(P("dp", None, None), P(), P(), P("tp", None), row_spec, row_spec),
                         out_specs=(row_spec, row_spec, P("dp"), row_spec), check_vma=False)
```

```python
import functools

import jax
import jax.numpy as jnp
from jax import lax
from jax.experimental import pallas as pl
from jax.experimental.pallas import tpu as pltpu
from jax.sharding import PartitionSpec as P

OPT_VOCAB = 50272
LN_EPS = 1e-5

TILE = 256
CHUNK = 256
PIECE = 32
LANES = 128
RING = 8
FIRST = 3
SPLIT = 4
PARTS = 6
LAST_PARTS = 9
HID_PARTS = 8
NORM_ROWS = 32
HEAD_VMEM = 52 << 20
SMALL_VMEM = 1 << 20
F32 = jnp.float32


def head_kernel(hid_hbm, gain_hbm, bias_hbm, emb_hbm, tgt_hbm, stats_ref,
                h, ring, z, gain, bias, tgt, mean_b, rstd_b, part, m8, s8, t8, small_sem, hid_sem, ring_sem,
                first_sem, last_sem):
    tokens, width = h.shape
    rows = emb_hbm.shape[0]
    n_chunks = rows // CHUNK
    passes = width // (2 * TILE)
    hid_rows = tokens // HID_PARTS
    base = lax.axis_index("tp") * rows

    def hid_copy(i):
        at = pl.ds(i * hid_rows, hid_rows)
        return pltpu.make_async_copy(hid_hbm.at[0, at], h.at[at], hid_sem.at[i])

    def chunk_copy(c):
        slot = lax.rem(c, RING)
        return pltpu.make_async_copy(emb_hbm.at[pl.ds(c * CHUNK, CHUNK)], ring.at[slot], ring_sem.at[slot])

    def start_chunk(c):
        n = CHUNK // SPLIT
        slot = lax.rem(c, RING)
        for i in range(SPLIT):
            pltpu.make_async_copy(emb_hbm.at[pl.ds(c * CHUNK + i * n, n)], ring.at[slot, pl.ds(i * n, n)],
                                  ring_sem.at[slot]).start(priority=1)

    def part_copy(c, i, n, sem):
        cols = pl.ds(i * (width // n), width // n)
        return pltpu.make_async_copy(
            emb_hbm.at[pl.ds(c * CHUNK, CHUNK), cols], ring.at[lax.rem(c, RING), :, cols], sem)

    def first_copy(e, i):
        return part_copy(e, i, PARTS, first_sem.at[e, i])

    def last_copy(e, i):
        return part_copy(n_chunks - 2 + e, i, LAST_PARTS, last_sem.at[e, i])

    small = [pltpu.make_async_copy(src, dst, small_sem.at[i]) for i, (src, dst) in enumerate(
        ((gain_hbm, gain), (bias_hbm, bias), (tgt_hbm, tgt)))]

    for i in range(HID_PARTS):
        hid_copy(i).start()
    for copy in small:
        copy.start()
    early = list(range(FIRST, RING))

    def lane_sum(r, n, fn):
        acc = [jnp.zeros((n, LANES), F32) for _ in range(2)]
        for c in range(width // LANES):
            acc[c % 2] += fn(h[pl.ds(r, n), pl.ds(c * LANES, LANES)].astype(F32))
        return acc[0] + acc[1]

    group = 16

    def groups(i):
        return [i * hid_rows + g * group for g in range(hid_rows // group)]

    def mean_rows(i):
        for r in groups(i):
            part[pl.ds(r, group)] = lane_sum(r, group, lambda x: x)
        at = pl.ds(i * hid_rows, hid_rows)
        mean = jnp.sum(part[at], axis=-1, keepdims=True) * (1.0 / width)
        mean_b[at] = jnp.broadcast_to(mean, (hid_rows, LANES))

    def var_sums(i):
        for r in groups(i):
            mean = mean_b[pl.ds(r, group)]
            rstd_b[pl.ds(r, group)] = lane_sum(r, group, lambda x: (x - mean) * (x - mean))

    def var_rows(i):
        at = pl.ds(i * hid_rows, hid_rows)
        var = jnp.sum(rstd_b[at], axis=-1, keepdims=True) * (1.0 / width)
        rstd_b[at] = jnp.broadcast_to(lax.rsqrt(var + LN_EPS), (hid_rows, LANES))

    for i in range(HID_PARTS):
        hid_copy(i).wait()
        if i == 0:
            for k in range(PARTS):
                for e in range(FIRST):
                    first_copy(e, k).start(priority=1)
        if i > 1:
            var_rows(i - 2)
        mean_rows(i)
        if i:
            var_sums(i - 1)
    start_chunk(early.pop(0))
    var_rows(HID_PARTS - 2)
    var_sums(HID_PARTS - 1)
    var_rows(HID_PARTS - 1)

    for copy in small:
        copy.wait()
    m8[...] = jnp.full_like(m8, jnp.finfo(F32).min)
    s8[...] = jnp.zeros_like(s8)
    t8[...] = jnp.zeros_like(t8)

    def normalize(k, r=0, n=tokens):
        at, cols = pl.ds(r, n), pl.ds(k * TILE, TILE)
        wide = lambda x: jnp.concatenate([x] * (TILE // LANES), axis=1)
        x = h[at, cols].astype(F32)
        x = (x - wide(mean_b[at])) * wide(rstd_b[at]) * gain[:, cols] + bias[:, cols]
        h[at, cols] = x.astype(h.dtype)

    def matmuls(*accs):
        n_piece = CHUNK // PIECE
        accs = [[accs[(w * 2 + q) * n_piece:(w * 2 + q + 1) * n_piece] for q in range(2)] for w in range(4)]

        for which in accs:
            for q in which:
                for acc in q:
                    z[pl.ds(0, PIECE)] = pltpu.matmul_pop(acc)

        def push(j, q):
            cols = pl.ds((2 * j + q) * TILE, TILE)
            pltpu.matmul_push_rhs(h[:, cols], staging_register=j % 2, mxu_index=q, transpose=True)

        def accumulate(chunks, sets, j):
            def step(c, which, p, q):
                lhs = ring[lax.rem(c, RING), pl.ds(p * PIECE, PIECE), pl.ds((2 * j + q) * TILE, TILE)]
                pltpu.matmul_acc_lhs(
                    accs[which][q][p], lhs, load_staged_rhs=j % 2 if which == sets[0] and p == 0 else None)
            return [functools.partial(step, c, which, p, q)
                    for c, which in zip(chunks, sets) for p in range(n_piece) for q in range(2)]

        def drain(c, which, p):
            offset = base + c * CHUNK
            target = tgt[...] - offset
            limit = OPT_VOCAB - offset
            shape = (PIECE // 8, 8, tokens)
            logits = pltpu.matmul_pop(accs[which][0][p]) + pltpu.matmul_pop(accs[which][1][p])
            row = lax.broadcasted_iota(jnp.int32, logits.shape, 0) + p * PIECE
            logits = jnp.where(row < limit, logits, -jnp.inf)
            z[pl.ds(p * PIECE, PIECE)] = logits
            m8[1] = jnp.maximum(m8[1], jnp.max(logits.reshape(shape), axis=0))
            t8[...] += jnp.sum(jnp.where(row == target, logits, 0.0).reshape(shape), axis=0)

        def exps(p):
            top = m8[1]
            total = s8[...]
            if p == 0:
                total = total * jnp.exp(m8[0] - top)
                m8[0] = top
            e = jnp.exp(z[pl.ds(p * PIECE, PIECE)].reshape(PIECE // 8, 8, tokens) - top[None])
            s8[...] = total + jnp.sum(e, axis=0)

        def absorb(c, which):
            return [functools.partial(drain, c, which, p) for p in range(n_piece)] + [
                functools.partial(exps, p) for p in range(n_piece)]

        def sweep(chunks, sets, beside=(), wait=None, parts=PARTS, norm=False, last=False):
            beside = list(beside)
            per_pass = pl.cdiv(len(beside), passes - 3)
            for j in range(passes):
                if wait is not None and j % (passes // parts) == 0:
                    wait(j // (passes // parts))
                def push_next():
                    for q in range(2):
                        if not (last and j + 1 == passes):
                            push((j + 1) % passes, q)

                steps = accumulate(chunks, sets, j)
                if norm and j + 1 < passes:
                    cut = len(steps) * 2 // 3
                    groups = [(2 * (j + 1) + q, r) for q in range(2) for r in range(0, tokens, NORM_ROWS)]
                    for i, step in enumerate(steps):
                        for k, r in groups[i * len(groups) // cut:(i + 1) * len(groups) // cut]:
                            normalize(k, r, NORM_ROWS)
                        if i == cut:
                            push_next()
                        step()
                else:
                    push_next()
                    for step in steps:
                        step()
                if j >= 2:
                    for step in beside[(j - 2) * per_pass:(j - 1) * per_pass]:
                        step()

        def first_wait(i):
            for e in range(FIRST):
                first_copy(e, i).wait()
            for _ in range(len(early) - (PARTS - 1 - i) * len(early) // (PARTS - i)):
                start_chunk(early.pop(0))

        def last_wait(i):
            for e in range(2):
                last_copy(e, i).wait()

        for k in range(2):
            normalize(k)
        for q in range(2):
            push(0, q)
        sweep(range(FIRST), range(FIRST), wait=first_wait, norm=True)
        for step in absorb(0, 0):
            step()
        for c in range(RING, RING + FIRST - 2):
            start_chunk(c)

        def pair(c, sets, old, refill=True):
            for e in range(2):
                chunk_copy(c + e).wait()
            if refill:
                @pl.when(c + RING < n_chunks)
                def _():
                    for e in range(2):
                        start_chunk(c - 2 + e + RING)

                @pl.when(c + RING == n_chunks)
                def _():
                    for i in range(LAST_PARTS):
                        for e in range(2):
                            last_copy(e, i).start(priority=1)
            sweep((c, c + 1), sets, absorb(c - 2, old[0]) + absorb(c - 1, old[1]))

        def two_pairs(i, carry):
            c = FIRST + 4 * i
            pair(c, (3, 0), (1, 2))
            pair(c + 2, (1, 2), (3, 0))
            return carry

        lax.fori_loop(0, (n_chunks - FIRST) // 4, two_pairs, 0)
        c = n_chunks - 2
        sweep((c, c + 1), (3, 0), absorb(c - 2, 1) + absorb(c - 1, 2), wait=last_wait, parts=LAST_PARTS,
              last=True)
        for step in absorb(c, 3) + absorb(c + 1, 0):
            step()

    pl.run_scoped(matmuls, *[pltpu.ACC(q)((PIECE, TILE), F32)
                             for _ in range(4) for q in range(2) for _ in range(CHUNK // PIECE)])

    top = jnp.max(m8[0], axis=0, keepdims=True)
    total = jnp.sum(s8[...] * jnp.exp(m8[0] - top), axis=0, keepdims=True)
    picked = jnp.sum(t8[...], axis=0, keepdims=True)
    stats_ref[...] = jnp.concatenate([top, total, picked], axis=1)


def exchange_kernel(n_tp, stats_ref, out_ref, box, send_sem, recv_sem):
    me = lax.axis_index("tp")

    def peer(d):
        return lax.rem(me + d, n_tp)

    def exchange(d, slot):
        return pltpu.make_async_remote_copy(
            src_ref=stats_ref, dst_ref=box.at[slot], send_sem=send_sem.at[d], recv_sem=recv_sem.at[slot],
            device_id={"tp": peer(d)}, device_id_type=pl.DeviceIdType.MESH)

    barrier = pltpu.get_barrier_semaphore()
    for d in range(1, n_tp):
        pl.semaphore_signal(barrier, inc=1, device_id={"tp": peer(d)}, device_id_type=pl.DeviceIdType.MESH)
    pl.semaphore_wait(barrier, n_tp - 1)
    for d in range(1, n_tp):
        exchange(d, me).start()
    box[me] = stats_ref[...]
    for d in range(1, n_tp):
        exchange(d, peer(d)).wait_recv()
    out_ref[...] = box[...]
    for d in range(1, n_tp):
        exchange(d, me).wait_send()


def finish_kernel(box, mask, norm_ref, logp_ref, seq_ref, top_ref):
    n_tp, _, width = box.shape
    tokens = width // 3
    boxes = [box[i] for i in range(n_tp)]
    top = functools.reduce(jnp.maximum, [x[:, :tokens] for x in boxes])
    total = sum(x[:, tokens:2 * tokens] * jnp.exp(x[:, :tokens] - top) for x in boxes)
    picked = sum(x[:, 2 * tokens:] for x in boxes)
    log_norm = top + jnp.log(total)
    token_logp = (picked - log_norm) * mask[...].astype(F32)
    norm_ref[...] = log_norm
    logp_ref[...] = token_logp
    top_ref[...] = top - log_norm
    seq_ref[...] = jnp.broadcast_to(jnp.sum(token_logp, axis=-1, keepdims=True), seq_ref.shape)


def solution(mesh):
    n_tp = mesh.shape["tp"]

    def local_part(hidden, ln_gain, ln_bias, embedding, targets, score_mask):
        prompts, tokens, width = hidden.shape
        rows = embedding.shape[0]
        n_chunks = rows // CHUNK
        assert prompts == 1 and tokens == TILE and rows % CHUNK == 0
        assert width % (2 * TILE * PARTS) == 0 and width % (2 * TILE * LAST_PARTS) == 0
        assert (n_chunks - FIRST) % 4 == 2 and n_chunks > RING + FIRST + 2
        row = jax.ShapeDtypeStruct((prompts, tokens), F32)
        stats = pl.pallas_call(
            head_kernel,
            out_shape=jax.ShapeDtypeStruct((1, 3 * tokens), F32),
            in_specs=[pl.BlockSpec(memory_space=pl.ANY)] * 5,
            out_specs=pl.BlockSpec(memory_space=pltpu.VMEM),
            scratch_shapes=[
                pltpu.VMEM((tokens, width), hidden.dtype),
                pltpu.VMEM((RING, CHUNK, width), embedding.dtype),
                pltpu.VMEM((CHUNK, tokens), F32),
                pltpu.VMEM((1, width), F32),
                pltpu.VMEM((1, width), F32),
                pltpu.VMEM((1, tokens), jnp.int32),
                pltpu.VMEM((tokens, LANES), F32),
                pltpu.VMEM((tokens, LANES), F32),
                pltpu.VMEM((tokens, LANES), F32),
                pltpu.VMEM((2, 8, tokens), F32),
                pltpu.VMEM((8, tokens), F32),
                pltpu.VMEM((8, tokens), F32),
                pltpu.SemaphoreType.DMA((3,)),
                pltpu.SemaphoreType.DMA((HID_PARTS,)),
                pltpu.SemaphoreType.DMA((RING,)),
                pltpu.SemaphoreType.DMA((FIRST, PARTS)),
                pltpu.SemaphoreType.DMA((2, LAST_PARTS)),
            ],
            compiler_params=pltpu.CompilerParams(
                vmem_limit_bytes=HEAD_VMEM),
            name="head",
        )(*[pltpu.with_memory_space_constraint(x, pltpu.HBM) for x in (
            hidden, ln_gain.reshape(1, width), ln_bias.reshape(1, width), embedding, targets)])
        vmem = pl.BlockSpec(memory_space=pltpu.VMEM)
        boxes = pl.pallas_call(
            functools.partial(exchange_kernel, n_tp),
            out_shape=jax.ShapeDtypeStruct((n_tp, 1, 3 * tokens), F32),
            in_specs=[vmem],
            out_specs=vmem,
            scratch_shapes=[
                pltpu.VMEM((n_tp, 1, 3 * tokens), F32),
                pltpu.SemaphoreType.DMA((n_tp,)),
                pltpu.SemaphoreType.DMA((n_tp,)),
            ],
            compiler_params=pltpu.CompilerParams(
                collective_id=0, has_side_effects=True, vmem_limit_bytes=SMALL_VMEM),
            name="exchange",
        )(stats)
        log_norm, token_logp, seq, top_logp = pl.pallas_call(
            finish_kernel,
            out_shape=(row, row, jax.ShapeDtypeStruct((prompts, LANES), F32), row),
            in_specs=[vmem] * 2,
            out_specs=[vmem] * 4,
            compiler_params=pltpu.CompilerParams(vmem_limit_bytes=SMALL_VMEM),
            name="finish",
        )(boxes, score_mask)
        return log_norm, token_logp, seq[:, 0], top_logp

    row_spec = P("dp", None)
    return jax.shard_map(local_part, mesh=mesh,
                         in_specs=(P("dp", None, None), P(), P(), P("tp", None), row_spec, row_spec),
                         out_specs=(row_spec, row_spec, P("dp"), row_spec), check_vma=False)
```

```python
import functools

import jax
import jax.numpy as jnp
from jax import lax
from jax.experimental import pallas as pl
from jax.experimental.pallas import tpu as pltpu
from jax.sharding import PartitionSpec as P

OPT_VOCAB = 50272
LN_EPS = 1e-5

TILE = 256
CHUNK = 256
PIECE = 32
LANES = 128
RING = 8
FIRST = 3
PARTS = 6
HID_PARTS = 8
NORM_ROWS = 32
HEAD_VMEM = 52 << 20
SMALL_VMEM = 1 << 20
F32 = jnp.float32


def head_kernel(hid_hbm, gain_hbm, bias_hbm, emb_hbm, tgt_hbm, stats_ref,
                h, ring, z, gain, bias, tgt, mean_b, rstd_b, part, m8, s8, t8, small_sem, hid_sem, ring_sem,
                first_sem, last_sem):
    tokens, width = h.shape
    rows = emb_hbm.shape[0]
    n_chunks = rows // CHUNK
    passes = width // (2 * TILE)
    part_width = width // PARTS
    part_passes = passes // PARTS
    hid_rows = tokens // HID_PARTS
    base = lax.axis_index("tp") * rows

    def hid_copy(i):
        at = pl.ds(i * hid_rows, hid_rows)
        return pltpu.make_async_copy(hid_hbm.at[0, at], h.at[at], hid_sem.at[i])

    def chunk_copy(c):
        slot = lax.rem(c, RING)
        return pltpu.make_async_copy(emb_hbm.at[pl.ds(c * CHUNK, CHUNK)], ring.at[slot], ring_sem.at[slot])

    def part_copy(c, i, sem):
        cols = pl.ds(i * part_width, part_width)
        return pltpu.make_async_copy(
            emb_hbm.at[pl.ds(c * CHUNK, CHUNK), cols], ring.at[lax.rem(c, RING), :, cols], sem)

    def first_copy(e, i):
        return part_copy(e, i, first_sem.at[e, i])

    def last_copy(e, i):
        return part_copy(n_chunks - 2 + e, i, last_sem.at[e, i])

    small = [pltpu.make_async_copy(src, dst, small_sem.at[i]) for i, (src, dst) in enumerate(
        ((gain_hbm, gain), (bias_hbm, bias), (tgt_hbm, tgt)))]

    for i in range(HID_PARTS):
        hid_copy(i).start()
    for copy in small:
        copy.start()
    early = list(range(FIRST, RING))

    def lane_sum(r, n, fn):
        acc = [jnp.zeros((n, LANES), F32) for _ in range(2)]
        for c in range(width // LANES):
            acc[c % 2] += fn(h[pl.ds(r, n), pl.ds(c * LANES, LANES)].astype(F32))
        return acc[0] + acc[1]

    group = 16

    def groups(i):
        return [i * hid_rows + g * group for g in range(hid_rows // group)]

    def mean_rows(i):
        for r in groups(i):
            part[pl.ds(r, group)] = lane_sum(r, group, lambda x: x)
        at = pl.ds(i * hid_rows, hid_rows)
        mean = jnp.sum(part[at], axis=-1, keepdims=True) * (1.0 / width)
        mean_b[at] = jnp.broadcast_to(mean, (hid_rows, LANES))

    def var_sums(i):
        for r in groups(i):
            mean = mean_b[pl.ds(r, group)]
            rstd_b[pl.ds(r, group)] = lane_sum(r, group, lambda x: (x - mean) * (x - mean))

    def var_rows(i):
        at = pl.ds(i * hid_rows, hid_rows)
        var = jnp.sum(rstd_b[at], axis=-1, keepdims=True) * (1.0 / width)
        rstd_b[at] = jnp.broadcast_to(lax.rsqrt(var + LN_EPS), (hid_rows, LANES))

    for i in range(HID_PARTS):
        hid_copy(i).wait()
        if i == 0:
            for k in range(PARTS):
                for e in range(FIRST):
                    first_copy(e, k).start()
        if i > 1:
            var_rows(i - 2)
        mean_rows(i)
        if i:
            var_sums(i - 1)
    chunk_copy(early.pop(0)).start()
    var_rows(HID_PARTS - 2)
    var_sums(HID_PARTS - 1)
    var_rows(HID_PARTS - 1)

    for copy in small:
        copy.wait()
    m8[...] = jnp.full_like(m8, jnp.finfo(F32).min)
    s8[...] = jnp.zeros_like(s8)
    t8[...] = jnp.zeros_like(t8)

    def normalize(k, r=0, n=tokens):
        at, cols = pl.ds(r, n), pl.ds(k * TILE, TILE)
        wide = lambda x: jnp.concatenate([x] * (TILE // LANES), axis=1)
        x = h[at, cols].astype(F32)
        x = (x - wide(mean_b[at])) * wide(rstd_b[at]) * gain[:, cols] + bias[:, cols]
        h[at, cols] = x.astype(h.dtype)

    def matmuls(*accs):
        n_piece = CHUNK // PIECE
        accs = [[accs[(w * 2 + q) * n_piece:(w * 2 + q + 1) * n_piece] for q in range(2)] for w in range(4)]

        for which in accs:
            for q in which:
                for acc in q:
                    z[pl.ds(0, PIECE)] = pltpu.matmul_pop(acc)

        def push(j, q):
            cols = pl.ds((2 * j + q) * TILE, TILE)
            pltpu.matmul_push_rhs(h[:, cols], staging_register=j % 2, mxu_index=q, transpose=True)

        def accumulate(chunks, sets, j):
            def step(c, which, p, q):
                lhs = ring[lax.rem(c, RING), pl.ds(p * PIECE, PIECE), pl.ds((2 * j + q) * TILE, TILE)]
                pltpu.matmul_acc_lhs(
                    accs[which][q][p], lhs, load_staged_rhs=j % 2 if which == sets[0] and p == 0 else None)
            return [functools.partial(step, c, which, p, q)
                    for c, which in zip(chunks, sets) for p in range(n_piece) for q in range(2)]

        def drain(c, which, p):
            offset = base + c * CHUNK
            target = tgt[...] - offset
            limit = OPT_VOCAB - offset
            shape = (PIECE // 8, 8, tokens)
            logits = pltpu.matmul_pop(accs[which][0][p]) + pltpu.matmul_pop(accs[which][1][p])
            row = lax.broadcasted_iota(jnp.int32, logits.shape, 0) + p * PIECE
            logits = jnp.where(row < limit, logits, -jnp.inf)
            z[pl.ds(p * PIECE, PIECE)] = logits
            m8[1] = jnp.maximum(m8[1], jnp.max(logits.reshape(shape), axis=0))
            t8[...] += jnp.sum(jnp.where(row == target, logits, 0.0).reshape(shape), axis=0)

        def exps(p):
            top = m8[1]
            total = s8[...]
            if p == 0:
                total = total * jnp.exp(m8[0] - top)
                m8[0] = top
            e = jnp.exp(z[pl.ds(p * PIECE, PIECE)].reshape(PIECE // 8, 8, tokens) - top[None])
            s8[...] = total + jnp.sum(e, axis=0)

        def absorb(c, which):
            return [functools.partial(drain, c, which, p) for p in range(n_piece)] + [
                functools.partial(exps, p) for p in range(n_piece)]

        def sweep(chunks, sets, beside=(), wait=None, norm=False, last=False):
            beside = list(beside)
            per_pass = pl.cdiv(len(beside), passes - 3)
            for j in range(passes):
                if wait is not None and j % part_passes == 0:
                    wait(j // part_passes)
                def push_next():
                    for q in range(2):
                        if not (last and j + 1 == passes):
                            push((j + 1) % passes, q)

                steps = accumulate(chunks, sets, j)
                if norm and j + 1 < passes:
                    cut = len(steps) * 2 // 3
                    groups = [(2 * (j + 1) + q, r) for q in range(2) for r in range(0, tokens, NORM_ROWS)]
                    for i, step in enumerate(steps):
                        for k, r in groups[i * len(groups) // cut:(i + 1) * len(groups) // cut]:
                            normalize(k, r, NORM_ROWS)
                        if i == cut:
                            push_next()
                        step()
                else:
                    push_next()
                    for step in steps:
                        step()
                if j >= 2:
                    for step in beside[(j - 2) * per_pass:(j - 1) * per_pass]:
                        step()

        def first_wait(i):
            for e in range(FIRST):
                first_copy(e, i).wait()
            for _ in range(len(early) - (PARTS - 1 - i) * len(early) // (PARTS - i)):
                chunk_copy(early.pop(0)).start()

        def last_wait(i):
            for e in range(2):
                last_copy(e, i).wait()

        for k in range(2):
            normalize(k)
        for q in range(2):
            push(0, q)
        sweep(range(FIRST), range(FIRST), wait=first_wait, norm=True)
        for step in absorb(0, 0):
            step()
        for c in range(RING, RING + FIRST - 2):
            chunk_copy(c).start()

        def pair(c, sets, old, refill=True):
            for e in range(2):
                chunk_copy(c + e).wait()
            if refill:
                @pl.when(c + RING < n_chunks)
                def _():
                    for e in range(2):
                        chunk_copy(c - 2 + e + RING).start()

                @pl.when(c + RING == n_chunks)
                def _():
                    for i in range(PARTS):
                        for e in range(2):
                            last_copy(e, i).start()
            sweep((c, c + 1), sets, absorb(c - 2, old[0]) + absorb(c - 1, old[1]))

        def two_pairs(i, carry):
            c = FIRST + 4 * i
            pair(c, (3, 0), (1, 2))
            pair(c + 2, (1, 2), (3, 0))
            return carry

        lax.fori_loop(0, (n_chunks - FIRST) // 4, two_pairs, 0)
        c = n_chunks - 2
        sweep((c, c + 1), (3, 0), absorb(c - 2, 1) + absorb(c - 1, 2), wait=last_wait, last=True)
        for step in absorb(c, 3) + absorb(c + 1, 0):
            step()

    pl.run_scoped(matmuls, *[pltpu.ACC(q)((PIECE, TILE), F32)
                             for _ in range(4) for q in range(2) for _ in range(CHUNK // PIECE)])

    top = jnp.max(m8[0], axis=0, keepdims=True)
    total = jnp.sum(s8[...] * jnp.exp(m8[0] - top), axis=0, keepdims=True)
    picked = jnp.sum(t8[...], axis=0, keepdims=True)
    stats_ref[...] = jnp.concatenate([top, total, picked], axis=1)


def exchange_kernel(n_tp, stats_ref, out_ref, box, send_sem, recv_sem):
    me = lax.axis_index("tp")

    def peer(d):
        return lax.rem(me + d, n_tp)

    def exchange(d, slot):
        return pltpu.make_async_remote_copy(
            src_ref=stats_ref, dst_ref=box.at[slot], send_sem=send_sem.at[d], recv_sem=recv_sem.at[slot],
            device_id={"tp": peer(d)}, device_id_type=pl.DeviceIdType.MESH)

    barrier = pltpu.get_barrier_semaphore()
    for d in range(1, n_tp):
        pl.semaphore_signal(barrier, inc=1, device_id={"tp": peer(d)}, device_id_type=pl.DeviceIdType.MESH)
    pl.semaphore_wait(barrier, n_tp - 1)
    for d in range(1, n_tp):
        exchange(d, me).start()
    box[me] = stats_ref[...]
    for d in range(1, n_tp):
        exchange(d, peer(d)).wait_recv()
    out_ref[...] = box[...]
    for d in range(1, n_tp):
        exchange(d, me).wait_send()


def finish_kernel(box, mask, norm_ref, logp_ref, seq_ref, top_ref):
    n_tp, _, width = box.shape
    tokens = width // 3
    boxes = [box[i] for i in range(n_tp)]
    top = functools.reduce(jnp.maximum, [x[:, :tokens] for x in boxes])
    total = sum(x[:, tokens:2 * tokens] * jnp.exp(x[:, :tokens] - top) for x in boxes)
    picked = sum(x[:, 2 * tokens:] for x in boxes)
    log_norm = top + jnp.log(total)
    token_logp = (picked - log_norm) * mask[...].astype(F32)
    norm_ref[...] = log_norm
    logp_ref[...] = token_logp
    top_ref[...] = top - log_norm
    seq_ref[...] = jnp.broadcast_to(jnp.sum(token_logp, axis=-1, keepdims=True), seq_ref.shape)


def solution(mesh):
    n_tp = mesh.shape["tp"]

    def local_part(hidden, ln_gain, ln_bias, embedding, targets, score_mask):
        prompts, tokens, width = hidden.shape
        rows = embedding.shape[0]
        n_chunks = rows // CHUNK
        assert prompts == 1 and tokens == TILE and rows % CHUNK == 0 and width % (2 * TILE * PARTS) == 0
        assert (n_chunks - FIRST) % 4 == 2 and n_chunks > RING + FIRST + 2
        row = jax.ShapeDtypeStruct((prompts, tokens), F32)
        stats = pl.pallas_call(
            head_kernel,
            out_shape=jax.ShapeDtypeStruct((1, 3 * tokens), F32),
            in_specs=[pl.BlockSpec(memory_space=pl.ANY)] * 5,
            out_specs=pl.BlockSpec(memory_space=pltpu.VMEM),
            scratch_shapes=[
                pltpu.VMEM((tokens, width), hidden.dtype),
                pltpu.VMEM((RING, CHUNK, width), embedding.dtype),
                pltpu.VMEM((CHUNK, tokens), F32),
                pltpu.VMEM((1, width), F32),
                pltpu.VMEM((1, width), F32),
                pltpu.VMEM((1, tokens), jnp.int32),
                pltpu.VMEM((tokens, LANES), F32),
                pltpu.VMEM((tokens, LANES), F32),
                pltpu.VMEM((tokens, LANES), F32),
                pltpu.VMEM((2, 8, tokens), F32),
                pltpu.VMEM((8, tokens), F32),
                pltpu.VMEM((8, tokens), F32),
                pltpu.SemaphoreType.DMA((3,)),
                pltpu.SemaphoreType.DMA((HID_PARTS,)),
                pltpu.SemaphoreType.DMA((RING,)),
                pltpu.SemaphoreType.DMA((FIRST, PARTS)),
                pltpu.SemaphoreType.DMA((2, PARTS)),
            ],
            compiler_params=pltpu.CompilerParams(
                vmem_limit_bytes=HEAD_VMEM),
            name="head",
        )(*[pltpu.with_memory_space_constraint(x, pltpu.HBM) for x in (
            hidden, ln_gain.reshape(1, width), ln_bias.reshape(1, width), embedding, targets)])
        vmem = pl.BlockSpec(memory_space=pltpu.VMEM)
        boxes = pl.pallas_call(
            functools.partial(exchange_kernel, n_tp),
            out_shape=jax.ShapeDtypeStruct((n_tp, 1, 3 * tokens), F32),
            in_specs=[vmem],
            out_specs=vmem,
            scratch_shapes=[
                pltpu.VMEM((n_tp, 1, 3 * tokens), F32),
                pltpu.SemaphoreType.DMA((n_tp,)),
                pltpu.SemaphoreType.DMA((n_tp,)),
            ],
            compiler_params=pltpu.CompilerParams(
                collective_id=0, has_side_effects=True, vmem_limit_bytes=SMALL_VMEM),
            name="exchange",
        )(stats)
        log_norm, token_logp, seq, top_logp = pl.pallas_call(
            finish_kernel,
            out_shape=(row, row, jax.ShapeDtypeStruct((prompts, LANES), F32), row),
            in_specs=[vmem] * 2,
            out_specs=[vmem] * 4,
            compiler_params=pltpu.CompilerParams(vmem_limit_bytes=SMALL_VMEM),
            name="finish",
        )(boxes, score_mask)
        return log_norm, token_logp, seq[:, 0], top_logp

    row_spec = P("dp", None)
    return jax.shard_map(local_part, mesh=mesh,
                         in_specs=(P("dp", None, None), P(), P(), P("tp", None), row_spec, row_spec),
                         out_specs=(row_spec, row_spec, P("dp"), row_spec), check_vma=False)
```
